8 devices in a mesh: rep: 2 (over y, z), dp: 4 (over x, core).
Axes of the slice: x: 2, y: 2, z: 1, core: 2. Of those that a mesh axis runs over, the one named last changes fastest.
Arguments:
- x: bfloat16 [8, 2048, 1024], P(('rep', 'dp')), parts along dimension 0
- dy: bfloat16 [8, 2048, 1024], P(('rep', 'dp')), parts along dimension 0
- w_gate: bfloat16 [2, 1024, 2560], replicated
- w_up: bfloat16 [2, 1024, 2560], replicated
- w_down: bfloat16 [2, 2560, 1024], replicated
- m_w_gate: float32 [2, 1024, 2560], replicated
- m_w_up: float32 [2, 1024, 2560], replicated
- m_w_down: float32 [2, 2560, 1024], replicated
- v_w_gate: float32 [2, 1024, 2560], replicated
- v_w_up: float32 [2, 1024, 2560], replicated
- v_w_down: float32 [2, 2560, 1024], replicated
Outputs:
- output 1: bfloat16 [4, 1024, 2560], P('rep'), parts along dimension 0
- output 2: bfloat16 [4, 1024, 2560], P('rep'), parts along dimension 0
- output 3: bfloat16 [4, 2560, 1024], P('rep'), parts along dimension 0
- output 4: float32 [4, 1024, 2560], P('rep'), parts along dimension 0
- output 5: float32 [4, 1024, 2560], P('rep'), parts along dimension 0
- output 6: float32 [4, 2560, 1024], P('rep'), parts along dimension 0
- output 7: float32 [4, 1024, 2560], P('rep'), parts along dimension 0
- output 8: float32 [4, 1024, 2560], P('rep'), parts along dimension 0
- output 9: float32 [4, 2560, 1024], P('rep'), parts along dimension 0
There are 2 independent parts. The reference program is written for one: setup_inputs(seed, part) draws one part's arguments, and reference() takes and returns one part's arrays. A program takes and returns all parts, laid end to end along the dimension named above; an argument that names none is the same for every part.
All inputs are finite; a program needn't handle non-finite values.
Results may differ from the reference program's by a relative error of at most 0.022.
Values are sent between devices in bfloat16 or wider.
A program may use at most 2.5 GiB of HBM per device.

```python
import jax
import jax.numpy as jnp
from jax import lax

SEQUENCES = 4
TOKENS = 2048
D = 1024
FF = 2560
LAYERS = 2
NAMES = ("w_gate", "w_up", "w_down")
SHAPES = {"w_gate": (LAYERS, D, FF), "w_up": (LAYERS, D, FF), "w_down": (LAYERS, FF, D)}


def bump(key, n, height):
    away = (jnp.arange(n, dtype=jnp.int32) - jax.random.randint(key, (), 0, n, jnp.int32)) % n
    return jnp.where(away < n // 8, height, 1.0)


def together(key, own, strength):
    shared = jax.random.normal(key, own.shape[1:], jnp.float32)
    return (own + strength * shared) * lax.rsqrt(1 + strength * strength)


def setup_inputs(seed: int = 0, part: int = 0) -> dict:
    kx, kdy, ka, kb, kz, kf, kh, kl, *keys = jax.random.split(jax.random.key(seed), 8 + 3 * len(NAMES))
    kx, kdy, ka, kb = (jax.random.fold_in(k, part) for k in (kx, kdy, ka, kb))
    kw, km, kv = (keys[i::3] for i in range(3))
    shape = (SEQUENCES, TOKENS, D)
    much_x, much_dy = jax.random.uniform(kz, (2,), jnp.float32, 0.0, 1.0)
    loud = 2.0 ** jax.random.uniform(jax.random.fold_in(kz, 1), (), jnp.float32, -1.0, 2.0)
    layers = 2.0 ** jax.random.uniform(kl, (LAYERS, 1, 1), jnp.float32, -1.0, 1.0)
    x = together(ka, jax.random.normal(kx, shape, jnp.float32), much_x) * bump(kf, D, 4.0)
    dy = together(kb, jax.random.normal(kdy, shape, jnp.float32), much_dy)
    drawn = {"x": x.astype(jnp.bfloat16), "dy": (loud * dy * (SEQUENCES * TOKENS) ** -0.5).astype(jnp.bfloat16)}
    for key, name in zip(kw, NAMES, strict=True):
        w = jax.random.normal(key, SHAPES[name], jnp.float32) * SHAPES[name][1] ** -0.5
        drawn[name] = (w * {"w_gate": 1.0, "w_up": bump(kh, FF, 4.0), "w_down": layers}[name]).astype(jnp.bfloat16)
    for key, name in zip(km, NAMES, strict=True):
        drawn[f"m_{name}"] = 0.1 * jax.random.normal(key, SHAPES[name], jnp.float32)
    for key, name in zip(kv, NAMES, strict=True):
        drawn[f"v_{name}"] = jax.random.uniform(key, SHAPES[name], jnp.float32, 0.005, 0.015)
    return drawn


def matmul(a, w):
    return jnp.dot(a, w, preferred_element_type=jnp.float32).astype(jnp.bfloat16)


def normed(h):
    wide = h.astype(jnp.float32)
    scale = lax.rsqrt(jnp.mean(wide**2, -1, keepdims=True) + 1e-6)
    return (wide * scale).astype(jnp.bfloat16)


def layer(h, w):
    a = normed(h)
    gate = jnp.dot(a, w["w_gate"], preferred_element_type=jnp.float32)
    up = jnp.dot(a, w["w_up"], preferred_element_type=jnp.float32)
    return h + matmul((jax.nn.silu(gate) * up).astype(jnp.bfloat16), w["w_down"])


def adamw(w, m, v, g):
    m = 0.9 * m + 0.1 * g
    v = 0.95 * v + 0.05 * g * g
    step = m * lax.rsqrt(v + 1e-8) + 0.1 * w
    return (w - 0.02 * step).astype(jnp.bfloat16), m, v


def clipped(gradients, sum_of_squares, count):
    factor = jnp.minimum(1.0, 0.5 * lax.rsqrt(sum_of_squares / count + 1e-30))
    return [g * factor for g in gradients]


def stack(weights, h):
    return lax.scan(lambda h, w: (layer(h, w), None), h, weights)[0]


def reference(x, dy, w_gate, w_up, w_down, m_w_gate, m_w_up, m_w_down, v_w_gate, v_w_up, v_w_down):
    weights = dict(zip(NAMES, (w_gate, w_up, w_down), strict=True))

    def take(so_far, sequence):
        h, by_y = sequence
        _, back = jax.vjp(lambda w: stack(w, h), weights)
        return jax.tree.map(lambda total, term: total + term.astype(jnp.float32), so_far, back(by_y)[0]), None

    none_yet = {name: jnp.zeros(w.shape, jnp.float32) for name, w in weights.items()}
    by_weights, _ = lax.scan(take, none_yet, (x, dy))
    gradients = [by_weights[name].astype(jnp.bfloat16).astype(jnp.float32) for name in NAMES]
    gradients = clipped(gradients, sum(jnp.sum(g * g) for g in gradients), sum(g.size for g in gradients))
    new = [
        adamw(w.astype(jnp.float32), m, v, g)
        for w, m, v, g in zip((w_gate, w_up, w_down), (m_w_gate, m_w_up, m_w_down), (v_w_gate, v_w_up, v_w_down), gradients, strict=True)
    ]
    return tuple(one[which] for which in range(3) for one in new)
```

```python
import jax
import jax.numpy as jnp
from jax import lax
from jax.experimental import pallas as pl
from jax.experimental.pallas import tpu as pltpu
from jax.sharding import PartitionSpec as P

F32, BF16 = jnp.float32, jnp.bfloat16
J = 256
ROWS = 512
LAG = 3
FAR = 2 * LAG + 2
VMEM_LIMIT = 67043328
MESH = pl.DeviceIdType.MESH


def dot(a, b):
    return jnp.dot(a, b, preferred_element_type=F32)


def dot_nt(a, b):
    return lax.dot_general(a, b, (((1,), (1,)), ((), ())), preferred_element_type=F32)


def norm_scale(wide):
    return lax.rsqrt(jnp.mean(wide**2, -1, keepdims=True) + 1e-6)


def gradients(x_hbm, dy_hbm, wg_hbm, wu_hbm, wd_hbm, g_hbm, ss_ref, h, a, at, dh, dht, acc0, acc1, act, dg, du, wg, wu, wd,
              grad, near, chip, far, total, ssv, ssr, w_sem, x_sem, s1_send, s1_recv, s2_send, s2_recv, s3_send, s3_recv, put_sem, ss_sem):
    tokens, d = h.shape
    blocks = tokens // ROWS
    n = wg_hbm.shape[2] // J
    steps = 2 * n
    half = d // 2
    me = lax.axis_index("dp")
    core = lax.rem(me, 2)
    partner = me + 1 - 2 * core
    across = lax.rem(me + 2, 4)

    def rows(r):
        return pl.ds(pl.multiple_of(r * ROWS, ROWS), ROWS)

    def weight_copies(f):
        slot, layer, j = lax.rem(f, 2), lax.rem(f // n, 2), lax.rem(f, n)
        cols = pl.ds(pl.multiple_of(j * J, J), J)
        return [
            pltpu.make_async_copy(wg_hbm.at[layer, :, cols], wg.at[slot], w_sem.at[0, slot]),
            pltpu.make_async_copy(wu_hbm.at[layer, :, cols], wu.at[slot], w_sem.at[1, slot]),
            pltpu.make_async_copy(wd_hbm.at[layer, cols, :], wd.at[slot], w_sem.at[2, slot]),
        ]

    def next_weights(f):
        for copy in weight_copies(f):
            copy.wait()

        @pl.when(f + 1 < 3 * n)
        def _():
            for copy in weight_copies(f + 1):
                copy.start()

        return lax.rem(f, 2)

    for copy in weight_copies(0):
        copy.start()
    get_x = pltpu.make_async_copy(x_hbm, h, x_sem.at[0])
    get_x.start()
    get_dy = pltpu.make_async_copy(dy_hbm, dh, x_sem.at[1])
    get_dy.start()
    barrier = pltpu.get_barrier_semaphore()
    for other in (partner, across):
        pl.semaphore_signal(barrier, inc=1, device_id={"dp": other}, device_id_type=MESH)
    pl.semaphore_wait(barrier, 2)
    ssv[...] = jnp.zeros_like(ssv)

    get_x.wait()

    def norm_block(r, _):
        wide = h[rows(r), :].astype(F32)
        a[rows(r), :] = (wide * norm_scale(wide)).astype(BF16)
        acc0[rows(r), :] = jnp.zeros((ROWS, d), F32)
        return 0

    lax.fori_loop(0, blocks, norm_block, 0)

    def forward(j, _):
        slot = next_weights(j)
        for r in range(blocks):
            here = pl.ds(r * ROWS, ROWS)
            block = a[here, :]
            gate = dot(block, wg[slot])
            up = dot(block, wu[slot])
            acc0[here, :] += dot((gate * jax.nn.sigmoid(gate) * up).astype(BF16), wd[slot])
        return 0

    lax.fori_loop(0, n, forward, 0)
    get_dy.wait()

    def turn(r, _):
        at[:, rows(r)] = a[rows(r), :].T
        dht[:, rows(r)] = dh[rows(r), :].T
        return 0

    def to_layer_1(r, _):
        new = h[rows(r), :] + acc0[rows(r), :].astype(BF16)
        h[rows(r), :] = new
        wide = new.astype(F32)
        a[rows(r), :] = (wide * norm_scale(wide)).astype(BF16)
        acc0[rows(r), :] = jnp.zeros((ROWS, d), F32)
        acc1[rows(r), :] = jnp.zeros((ROWS, d), F32)
        return turn(r, 0)

    lax.fori_loop(0, blocks, to_layer_1, 0)

    def to_layer_0(r, _):
        by_a = (acc0[rows(r), :].astype(BF16).astype(F32) + acc1[rows(r), :].astype(BF16).astype(F32)).astype(BF16).astype(F32)
        wide = h[rows(r), :].astype(F32)
        mean = jnp.mean(wide**2, -1, keepdims=True) + 1e-6
        scale = lax.rsqrt(mean)
        by_scale = jnp.sum(by_a * wide, -1, keepdims=True)
        by_wide = by_a * scale - wide * (by_scale * scale / mean * (1.0 / d))
        dh[rows(r), :] = (dh[rows(r), :].astype(F32) + by_wide.astype(BF16).astype(F32)).astype(BF16)
        return 0

    def again(r, _):
        wide = h[rows(r), :].astype(F32)
        a[rows(r), :] = (wide * norm_scale(wide)).astype(BF16)
        return turn(r, 0)

    def s1(t):
        slot = lax.rem(t, 2)
        return pltpu.make_async_remote_copy(
            src_ref=grad.at[:, pl.ds(pl.multiple_of((1 - core) * half, half), half), :], dst_ref=near.at[slot],
            send_sem=s1_send, recv_sem=s1_recv.at[slot], device_id={"dp": partner}, device_id_type=MESH)

    def s2(t):
        return pltpu.make_async_remote_copy(
            src_ref=chip.at[lax.rem(t, LAG + 1)], dst_ref=far.at[lax.rem(t, FAR)], send_sem=s2_send.at[lax.rem(t, LAG + 1)],
            recv_sem=s2_recv.at[lax.rem(t, FAR)], device_id={"dp": across}, device_id_type=MESH)

    def place(t, which):
        return g_hbm.at[t, :, pl.ds(pl.multiple_of(which * half, half), half), :]

    def s3(t):
        return pltpu.make_async_remote_copy(
            src_ref=total.at[lax.rem(t, 2)], dst_ref=place(t, core), send_sem=s3_send.at[lax.rem(t, 2)], recv_sem=s3_recv.at[t],
            device_id={"dp": partner}, device_id_type=MESH)

    def put(t):
        return pltpu.make_async_copy(total.at[lax.rem(t, 2)], place(t, core), put_sem.at[lax.rem(t, 2)])

    def step(t, _):
        @pl.when(t < steps)
        def _():
            @pl.when(t == n)
            def _():
                lax.fori_loop(0, blocks, to_layer_0, 0)
                again_x = pltpu.make_async_copy(x_hbm, h, x_sem.at[0])
                again_x.start()
                again_x.wait()
                lax.fori_loop(0, blocks, again, 0)

            slot = next_weights(n + t)

            def block(r, _):
                here = rows(r)
                gate = dot(a[here, :], wg[slot])
                up = dot(a[here, :], wu[slot])
                by_act = dot_nt(dh[here, :], wd[slot]).astype(BF16).astype(F32)
                s = jax.nn.sigmoid(gate)
                silu = gate * s
                act[here, :] = (silu * up).astype(BF16)
                du[here, :] = (by_act * silu).astype(BF16)
                dg[here, :] = (by_act * up * (s + silu * (1.0 - s))).astype(BF16)
                return 0

            lax.fori_loop(0, blocks, block, 0, unroll=2)

            def rest(r, _):
                here = rows(r)
                grad[0, here, :] = dot(at[here, :], dg[...]).astype(BF16)
                grad[1, here, :] = dot(at[here, :], du[...]).astype(BF16)
                grad[2, here, :] = dot(dht[here, :], act[...]).astype(BF16)
                return 0

            lax.fori_loop(0, d // ROWS, rest, 0)
            s1(t).start()

            @pl.when(t < n)
            def _():
                def back(r, _):
                    here = rows(r)
                    acc0[here, :] += dot_nt(dg[here, :], wg[slot])
                    acc1[here, :] += dot_nt(du[here, :], wu[slot])
                    return 0

                lax.fori_loop(0, blocks, back, 0)

            s1(t).wait()
            own = pl.ds(pl.multiple_of(core * half, half), half)
            for k in range(3):
                chip[lax.rem(t, LAG + 1), k] = (grad[k, own, :].astype(F32) + near[lax.rem(t, 2), k].astype(F32)).astype(BF16)
            s2(t).start()

        @pl.when(t >= LAG)
        def _():
            u = t - LAG

            @pl.when(u >= 2)
            def _():
                s3(u - 2).wait_send()
                put(u - 2).wait()

            s2(u).wait()
            for k in range(3):
                new = (chip[lax.rem(u, LAG + 1), k].astype(F32) + far[lax.rem(u, FAR), k].astype(F32)).astype(BF16)
                total[lax.rem(u, 2), k] = new
                wide = new.astype(F32)
                ssv[...] += jnp.sum((wide * wide).reshape(half // 8, 8, J), 0)
            s3(u).start()
            put(u).start()

        return 0

    lax.fori_loop(0, steps + LAG, step, 0)
    share = pltpu.make_async_remote_copy(
        src_ref=ssv, dst_ref=ssr, send_sem=ss_sem.at[0], recv_sem=ss_sem.at[1], device_id={"dp": partner}, device_id_type=MESH)
    share.start()
    for u in (steps - 2, steps - 1):
        s3(u).wait_send()
        put(u).wait()

    def arrived(t, _):
        s3(t).wait_recv()
        return 0

    lax.fori_loop(0, steps, arrived, 0)
    share.wait()
    ss_ref[...] = ssv[...] + ssr[...]


def call_gradients(x, dy, wg, wu, wd):
    tokens, d = x.shape
    n = wg.shape[2] // J
    half = d // 2
    hbm = pl.BlockSpec(memory_space=pl.ANY)
    dma = pltpu.SemaphoreType.DMA
    return pl.pallas_call(
        gradients,
        name="gradients",
        out_shape=(jax.ShapeDtypeStruct((2 * n, 3, d, J), BF16), jax.ShapeDtypeStruct((8, J), F32)),
        in_specs=[hbm] * 5,
        out_specs=(hbm, pl.BlockSpec(memory_space=pltpu.VMEM)),
        scratch_shapes=[
            pltpu.VMEM((tokens, d), BF16), pltpu.VMEM((tokens, d), BF16), pltpu.VMEM((d, tokens), BF16),
            pltpu.VMEM((tokens, d), BF16), pltpu.VMEM((d, tokens), BF16),
            pltpu.VMEM((tokens, d), F32), pltpu.VMEM((tokens, d), F32),
            pltpu.VMEM((tokens, J), BF16), pltpu.VMEM((tokens, J), BF16), pltpu.VMEM((tokens, J), BF16),
            pltpu.VMEM((2, d, J), BF16), pltpu.VMEM((2, d, J), BF16), pltpu.VMEM((2, J, d), BF16),
            pltpu.VMEM((3, d, J), BF16), pltpu.VMEM((2, 3, half, J), BF16), pltpu.VMEM((LAG + 1, 3, half, J), BF16),
            pltpu.VMEM((FAR, 3, half, J), BF16), pltpu.VMEM((2, 3, half, J), BF16),
            pltpu.VMEM((8, J), F32), pltpu.VMEM((8, J), F32),
            dma((3, 2)), dma((2,)), dma, dma((2,)), dma((LAG + 1,)), dma((FAR,)), dma((2,)), dma((2 * n,)), dma((2,)), dma((2,)),
        ],
        compiler_params=pltpu.CompilerParams(collective_id=0, has_side_effects=True, vmem_limit_bytes=VMEM_LIMIT),
    )(x, dy, wg, wu, wd)


def adamw(count, ss, g, wg, wu, wd, mg, mu, md, vg, vu, vd, *outs):
    squares = jnp.sum(jnp.sum(ss[...], 0, keepdims=True), 1, keepdims=True)
    factor = jnp.minimum(1.0, 0.5 * lax.rsqrt(squares / count + 1e-30))
    for k, (w, m, v) in enumerate(((wg, mg, vg), (wu, mu, vu), (wd, md, vd))):
        mine = g[0, k].astype(F32)
        mine = (mine.T if k == 2 else mine) * factor
        new_m = 0.9 * m[0] + 0.1 * mine
        new_v = 0.95 * v[0] + 0.05 * mine * mine
        w_out, m_out, v_out = outs[k], outs[3 + k], outs[6 + k]
        old = w[0].astype(F32)
        w_out[0] = (old - 0.02 * (new_m * lax.rsqrt(new_v + 1e-8) + 0.1 * old)).astype(BF16)
        m_out[0] = new_m
        v_out[0] = new_v


def call_adamw(ss, g, weights, m, v):
    layers, d, ff = weights[0].shape
    n = ff // J
    wide = pl.BlockSpec((1, d, J), lambda l, j: (l, 0, j))
    tall = pl.BlockSpec((1, J, d), lambda l, j: (l, j, 0))
    three = [wide, wide, tall]
    count = float(3 * layers * d * ff)
    return pl.pallas_call(
        lambda *refs: adamw(count, *refs),
        name="adamw",
        grid=(layers, n),
        out_shape=[jax.ShapeDtypeStruct(w.shape, t) for t in (BF16, F32, F32) for w in weights],
        in_specs=[pl.BlockSpec((8, J), lambda l, j: (0, 0)), pl.BlockSpec((1, 3, d, J), lambda l, j: ((layers - 1 - l) * n + j, 0, 0, 0))] + three * 3,
        out_specs=three * 3,
        compiler_params=pltpu.CompilerParams(vmem_limit_bytes=VMEM_LIMIT),
    )(ss, g, *weights, *m, *v)


def solution(mesh):
    def step(x, dy, *arrays):
        weights, m, v = (arrays[i : i + 3] for i in (0, 3, 6))
        g, ss = call_gradients(x[0], dy[0], *weights)
        return tuple(call_adamw(ss, g, weights, m, v))

    return jax.shard_map(
        step,
        mesh=mesh,
        in_specs=(P(("rep", "dp"), None, None),) * 2 + (P(None, None, None),) * 9,
        out_specs=(P("rep", None, None),) * 9,
        check_vma=False,
    )
```

```python
import jax
import jax.numpy as jnp
from jax import lax
from jax.experimental import pallas as pl
from jax.experimental.pallas import tpu as pltpu
from jax.sharding import PartitionSpec as P

F32, BF16 = jnp.float32, jnp.bfloat16
J = 256
ROWS = 512
VMEM_LIMIT = 67043328
MESH = pl.DeviceIdType.MESH


def dot(a, b):
    return jnp.dot(a, b, preferred_element_type=F32)


def dot_nt(a, b):
    return lax.dot_general(a, b, (((1,), (1,)), ((), ())), preferred_element_type=F32)


def norm_scale(wide):
    return lax.rsqrt(jnp.mean(wide**2, -1, keepdims=True) + 1e-6)


def gradients(x_hbm, dy_hbm, wg_hbm, wu_hbm, wd_hbm, g_hbm, ss_ref, h_hbm, far_h, far_dy, own_hbm, h, a, at, dh, dht, acc, act, dgu, wgu, wd,
              grad, mine, near, chip, far, total, ssv, ssr, w_sem, x_sem, own_sem, far_send, far_recv, s1_send, s1_recv, s2_send, s2_recv,
              s3_send, s3_recv, put_sem, ss_sem):
    tokens, d = h.shape
    blocks = tokens // ROWS
    n = wg_hbm.shape[2] // J
    half = d // 2
    me = lax.axis_index("dp")
    core = lax.rem(me, 2)
    partner = me + 1 - 2 * core
    across = lax.rem(me + 2, 4)

    def rows(r):
        return pl.ds(pl.multiple_of(r * ROWS, ROWS), ROWS)

    def half_of(which):
        return pl.ds(pl.multiple_of(which * half, half), half)

    def weight_copies(f):
        slot, layer, j = lax.rem(f, 2), lax.rem(f // n, 2), lax.rem(f, n)
        cols = pl.ds(pl.multiple_of(j * J, J), J)
        return [
            pltpu.make_async_copy(wg_hbm.at[layer, :, cols], wgu.at[slot, :, pl.ds(0, J)], w_sem.at[0, slot]),
            pltpu.make_async_copy(wu_hbm.at[layer, :, cols], wgu.at[slot, :, pl.ds(J, J)], w_sem.at[1, slot]),
            pltpu.make_async_copy(wd_hbm.at[layer, cols, :], wd.at[slot], w_sem.at[2, slot]),
        ]

    def next_weights(f):
        for copy in weight_copies(f):
            copy.wait()

        @pl.when(f + 1 < 4 * n)
        def _():
            for copy in weight_copies(f + 1):
                copy.start()

        return lax.rem(f, 2)

    def to_across(src, dst, k):
        return pltpu.make_async_remote_copy(
            src_ref=src, dst_ref=dst, send_sem=far_send.at[k], recv_sem=far_recv.at[k], device_id={"dp": across}, device_id_type=MESH)

    for copy in weight_copies(0):
        copy.start()
    get_x = pltpu.make_async_copy(x_hbm, h, x_sem.at[0])
    get_x.start()
    get_dy = pltpu.make_async_copy(dy_hbm, dh, x_sem.at[1])
    get_dy.start()
    barrier = pltpu.get_barrier_semaphore()
    for other in (partner, across):
        pl.semaphore_signal(barrier, inc=1, device_id={"dp": other}, device_id_type=MESH)
    pl.semaphore_wait(barrier, 2)
    send_dy = to_across(dy_hbm, far_dy, 0)
    send_dy.start()
    ssv[...] = jnp.zeros_like(ssv)
    get_x.wait()

    def first_norm(r, _):
        wide = h[rows(r), :].astype(F32)
        a[rows(r), :] = (wide * norm_scale(wide)).astype(BF16)
        acc[rows(r), :] = jnp.zeros((ROWS, d), F32)
        return 0

    lax.fori_loop(0, blocks, first_norm, 0)

    def forward(j, _):
        slot = next_weights(j)
        for r in range(blocks):
            here = pl.ds(r * ROWS, ROWS)
            both = dot(a[here, :], wgu[slot])
            gate, up = both[:, :J], both[:, J:]
            acc[here, :] += dot((gate * jax.nn.sigmoid(gate) * up).astype(BF16), wd[slot])
        return 0

    lax.fori_loop(0, n, forward, 0)

    def end_layer_0(r, _):
        h[rows(r), :] = h[rows(r), :] + acc[rows(r), :].astype(BF16)
        acc[rows(r), :] = jnp.zeros((ROWS, d), F32)
        return 0

    lax.fori_loop(0, blocks, end_layer_0, 0)
    keep_h = pltpu.make_async_copy(h, h_hbm, x_sem.at[0])
    keep_h.start()
    get_dy.wait()
    keep_h.wait()
    send_h = to_across(h_hbm, far_h, 1)
    send_h.start()

    def to_layer_0(r, _):
        by_a = acc[rows(r), :].astype(BF16).astype(F32)
        wide = h[rows(r), :].astype(F32)
        mean = jnp.mean(wide**2, -1, keepdims=True) + 1e-6
        scale = lax.rsqrt(mean)
        by_scale = jnp.sum(by_a * wide, -1, keepdims=True)
        by_wide = by_a * scale - wide * (by_scale * scale / mean * (1.0 / d))
        dh[rows(r), :] = (dh[rows(r), :].astype(F32) + by_wide.astype(BF16).astype(F32)).astype(BF16)
        return 0

    def begin(r, _):
        wide = h[rows(r), :].astype(F32)
        a[rows(r), :] = (wide * norm_scale(wide)).astype(BF16)
        at[:, rows(r)] = a[rows(r), :].T
        dht[:, rows(r)] = dh[rows(r), :].T
        return 0

    def s1(u):
        slot = lax.rem(u, 2)
        return pltpu.make_async_remote_copy(
            src_ref=grad.at[:, half_of(1 - core), :], dst_ref=near.at[slot],
            send_sem=s1_send, recv_sem=s1_recv.at[slot], device_id={"dp": partner}, device_id_type=MESH)

    def s2(j):
        return pltpu.make_async_remote_copy(
            src_ref=chip.at[j], dst_ref=far.at[j], send_sem=s2_send.at[j], recv_sem=s2_recv.at[j],
            device_id={"dp": across}, device_id_type=MESH)

    def s3(layer, j):
        slot, index = 2 * layer + lax.rem(j, 2), layer * n + j
        return pltpu.make_async_remote_copy(
            src_ref=total.at[slot], dst_ref=g_hbm.at[index, :, half_of(core), :], send_sem=s3_send.at[slot], recv_sem=s3_recv.at[index],
            device_id={"dp": partner}, device_id_type=MESH)

    def put(layer, j):
        slot = 2 * layer + lax.rem(j, 2)
        return pltpu.make_async_copy(total.at[slot], g_hbm.at[layer * n + j, :, half_of(core), :], put_sem.at[slot])

    def free_total(layer, j):
        @pl.when(j >= 2)
        def _():
            s3(layer, j - 2).wait_send()
            put(layer, j - 2).wait()

    def deliver(layer, j, new, k):
        total[2 * layer + lax.rem(j, 2), k] = new
        wide = new.astype(F32)
        ssv[...] += jnp.sum((wide * wide).reshape(half // 8, 8, J), 0)

    def keep(j):
        return pltpu.make_async_copy(grad, own_hbm.at[j], own_sem)

    def step(t, _):
        p, j = t // n, lax.rem(t, n)

        @pl.when(jnp.logical_and(p == 1, j == 0))
        def _():
            keep(n - 1).wait()
            lax.fori_loop(0, blocks, to_layer_0, 0)
            get = pltpu.make_async_copy(x_hbm, h, x_sem.at[0])
            get.start()
            get.wait()

        @pl.when(jnp.logical_and(p == 2, j == 0))
        def _():
            to_across(dy_hbm, far_dy, 0).wait()
            to_across(h_hbm, far_h, 1).wait()
            get = pltpu.make_async_copy(far_h, h, x_sem.at[0])
            get.start()
            get_too = pltpu.make_async_copy(far_dy, dh, x_sem.at[1])
            get_too.start()
            get.wait()
            get_too.wait()

        @pl.when(j == 0)
        def _():
            lax.fori_loop(0, blocks, begin, 0)

        slot = next_weights(n + t)

        @pl.when(p == 2)
        def _():
            pltpu.make_async_copy(own_hbm.at[j], mine, own_sem).start()

        def block(r, _):
            here = rows(r)
            both = dot(a[here, :], wgu[slot])
            gate, up = both[:, :J], both[:, J:]
            by_act = dot_nt(dh[here, :], wd[slot]).astype(BF16).astype(F32)
            s = jax.nn.sigmoid(gate)
            silu = gate * s
            act[here, :] = (silu * up).astype(BF16)
            dgu[here, J:] = (by_act * silu).astype(BF16)
            dgu[here, :J] = (by_act * up * (s + silu * (1.0 - s))).astype(BF16)
            return 0

        lax.fori_loop(0, blocks, block, 0, unroll=True)

        @pl.when(jnp.logical_and(p == 0, j > 0))
        def _():
            keep(j - 1).wait()

        def rest(i, _):
            here = half_of(lax.rem(1 - core + i, 2))
            both = dot(at[here, :], dgu[...]).astype(BF16)
            grad[0, here, :] = both[:, :J]
            grad[1, here, :] = both[:, J:]
            grad[2, here, :] = dot(dht[here, :], act[...]).astype(BF16)

            @pl.when(jnp.logical_and(i == 0, p == 2))
            def _():
                pltpu.make_async_copy(own_hbm.at[j], mine, own_sem).wait()
                for k in range(3):
                    grad[k, here, :] = (grad[k, here, :].astype(F32) + mine[k, here, :].astype(F32)).astype(BF16)

            @pl.when(jnp.logical_and(i == 0, p >= 1))
            def _():
                s1(t - n).start()

            return 0

        lax.fori_loop(0, 2, rest, 0)

        @pl.when(p == 0)
        def _():
            keep(j).start()

            def back(r, _):
                acc[rows(r), :] += dot_nt(dgu[rows(r), :], wgu[slot])
                return 0

            lax.fori_loop(0, blocks, back, 0, unroll=True)

        @pl.when(p == 1)
        def _():
            s1(t - n).wait()
            for k in range(3):
                chip[j, k] = (grad[k, half_of(core), :].astype(F32) + near[lax.rem(t - n, 2), k].astype(F32)).astype(BF16)
            s2(j).start()

        @pl.when(p == 2)
        def _():
            free_total(1, j)
            s1(t - n).wait()
            for k in range(3):
                new = grad[k, half_of(core), :].astype(F32) + mine[k, half_of(core), :].astype(F32)
                deliver(1, j, (new + near[lax.rem(t - n, 2), k].astype(F32)).astype(BF16), k)
            s3(1, j).start()
            put(1, j).start()
            free_total(0, j)
            s2(j).wait()
            for k in range(3):
                deliver(0, j, (chip[j, k].astype(F32) + far[j, k].astype(F32)).astype(BF16), k)
            s3(0, j).start()
            put(0, j).start()

        return 0

    lax.fori_loop(0, 3 * n, step, 0)
    share = pltpu.make_async_remote_copy(
        src_ref=ssv, dst_ref=ssr, send_sem=ss_sem.at[0], recv_sem=ss_sem.at[1], device_id={"dp": partner}, device_id_type=MESH)
    share.start()
    for layer in range(2):
        for j in (n - 2, n - 1):
            s3(layer, j).wait_send()
            put(layer, j).wait()

    def arrived(j, _):
        s3(0, j).wait_recv()
        s3(1, j).wait_recv()
        return 0

    lax.fori_loop(0, n, arrived, 0)
    share.wait()
    ss_ref[...] = ssv[...] + ssr[...]


def call_gradients(x, dy, wg, wu, wd):
    tokens, d = x.shape
    n = wg.shape[2] // J
    half = d // 2
    hbm = pl.BlockSpec(memory_space=pl.ANY)
    dma = pltpu.SemaphoreType.DMA
    part = (3, half, J)
    out = pl.pallas_call(
        gradients,
        name="gradients",
        out_shape=(
            jax.ShapeDtypeStruct((2 * n, 3, d, J), BF16), jax.ShapeDtypeStruct((8, J), F32),
            *[jax.ShapeDtypeStruct((tokens, d), BF16)] * 3, jax.ShapeDtypeStruct((n, 3, d, J), BF16),
        ),
        in_specs=[hbm] * 5,
        out_specs=(hbm, pl.BlockSpec(memory_space=pltpu.VMEM), hbm, hbm, hbm, hbm),
        scratch_shapes=[
            pltpu.VMEM((tokens, d), BF16), pltpu.VMEM((tokens, d), BF16), pltpu.VMEM((d, tokens), BF16),
            pltpu.VMEM((tokens, d), BF16), pltpu.VMEM((d, tokens), BF16),
            pltpu.VMEM((tokens, d), F32),
            pltpu.VMEM((tokens, J), BF16), pltpu.VMEM((tokens, 2 * J), BF16),
            pltpu.VMEM((2, d, 2 * J), BF16), pltpu.VMEM((2, J, d), BF16),
            pltpu.VMEM((3, d, J), BF16), pltpu.VMEM((3, d, J), BF16), pltpu.VMEM((2, *part), BF16), pltpu.VMEM((n, *part), BF16),
            pltpu.VMEM((n, *part), BF16), pltpu.VMEM((4, *part), BF16),
            pltpu.VMEM((8, J), F32), pltpu.VMEM((8, J), F32),
            dma((3, 2)), dma((2,)), dma, dma((2,)), dma((2,)), dma, dma((2,)), dma((n,)), dma((n,)), dma((4,)), dma((2 * n,)), dma((4,)), dma((2,)),
        ],
        compiler_params=pltpu.CompilerParams(collective_id=0, has_side_effects=True, vmem_limit_bytes=VMEM_LIMIT),
    )(x, dy, wg, wu, wd)
    return out[0], out[1]


def adamw(count, ss, g, wg, wu, wd, mg, mu, md, vg, vu, vd, *outs):
    squares = jnp.sum(jnp.sum(ss[...], 0, keepdims=True), 1, keepdims=True)
    factor = jnp.minimum(1.0, 0.5 * lax.rsqrt(squares / count + 1e-30))
    for k, (w, m, v) in enumerate(((wg, mg, vg), (wu, mu, vu), (wd, md, vd))):
        mine = g[0, k].astype(F32)
        mine = (mine.T if k == 2 else mine) * factor
        new_m = 0.9 * m[0] + 0.1 * mine
        new_v = 0.95 * v[0] + 0.05 * mine * mine
        w_out, m_out, v_out = outs[k], outs[3 + k], outs[6 + k]
        old = w[0].astype(F32)
        w_out[0] = (old - 0.02 * (new_m * lax.rsqrt(new_v + 1e-8) + 0.1 * old)).astype(BF16)
        m_out[0] = new_m
        v_out[0] = new_v


def call_adamw(ss, g, weights, m, v):
    layers, d, ff = weights[0].shape
    n = ff // J
    wide = pl.BlockSpec((1, d, J), lambda l, j: (l, 0, j))
    tall = pl.BlockSpec((1, J, d), lambda l, j: (l, j, 0))
    three = [wide, wide, tall]
    count = float(3 * layers * d * ff)
    return pl.pallas_call(
        lambda *refs: adamw(count, *refs),
        name="adamw",
        grid=(layers, n),
        out_shape=[jax.ShapeDtypeStruct(w.shape, t) for t in (BF16, F32, F32) for w in weights],
        in_specs=[pl.BlockSpec((8, J), lambda l, j: (0, 0)), pl.BlockSpec((1, 3, d, J), lambda l, j: (l * n + j, 0, 0, 0))] + three * 3,
        out_specs=three * 3,
        compiler_params=pltpu.CompilerParams(vmem_limit_bytes=VMEM_LIMIT),
    )(ss, g, *weights, *m, *v)


def solution(mesh):
    def step(x, dy, *arrays):
        weights, m, v = (arrays[i : i + 3] for i in (0, 3, 6))
        g, ss = call_gradients(x[0], dy[0], *weights)
        return tuple(call_adamw(ss, g, weights, m, v))

    return jax.shard_map(
        step,
        mesh=mesh,
        in_specs=(P(("rep", "dp"), None, None),) * 2 + (P(None, None, None),) * 9,
        out_specs=(P("rep", None, None),) * 9,
        check_vma=False,
    )
```

```python
import jax
import jax.numpy as jnp
from jax import lax
from jax.experimental import pallas as pl
from jax.experimental.pallas import tpu as pltpu
from jax.sharding import PartitionSpec as P

F32, BF16 = jnp.float32, jnp.bfloat16
J = 256
ROWS = 512
VMEM_LIMIT = 67043328
WIDE, TALL = 256, 64
HANDED = 28 * 2**20
MESH = pl.DeviceIdType.MESH


def dot(a, b):
    return jnp.dot(a, b, preferred_element_type=F32)


def dot_nt(a, b):
    return lax.dot_general(a, b, (((1,), (1,)), ((), ())), preferred_element_type=F32)


def norm_scale(wide):
    return lax.rsqrt(jnp.mean(wide**2, -1, keepdims=True) + 1e-6)


def gradients(x_hbm, dy_hbm, wg_hbm, wu_hbm, wd_hbm, md_hbm, g_hbm, gd_hbm, ss_ref, h_hbm, far_h, far_dy, own_hbm, h, a, at, dh, dht, acc, act, dgu, wgu, wd,
              grad, mine, near, chip, far, total, total_d, ssv, ssr, w_sem, x_sem, own_sem, far_send, far_recv, s1_send, s1_recv, s2_send, s2_recv,
              s3_send, s3_recv, put_sem, ss_sem, hand_sem):
    tokens, d = h.shape
    blocks = tokens // ROWS
    n = wg_hbm.shape[2] // J
    half = d // 2
    me = lax.axis_index("dp")
    core = lax.rem(me, 2)
    partner = me + 1 - 2 * core
    across = lax.rem(me + 2, 4)

    def rows(r):
        return pl.ds(pl.multiple_of(r * ROWS, ROWS), ROWS)

    def half_of(which):
        return pl.ds(pl.multiple_of(which * half, half), half)

    def weight_copies(f):
        slot, layer, j = lax.rem(f, 2), lax.rem(f // n, 2), lax.rem(f, n)
        cols = pl.ds(pl.multiple_of(j * J, J), J)
        return [
            pltpu.make_async_copy(wg_hbm.at[layer, :, cols], wgu.at[slot, :, pl.ds(0, J)], w_sem.at[0, slot]),
            pltpu.make_async_copy(wu_hbm.at[layer, :, cols], wgu.at[slot, :, pl.ds(J, J)], w_sem.at[1, slot]),
            pltpu.make_async_copy(wd_hbm.at[layer, cols, :], wd.at[slot], w_sem.at[2, slot]),
        ]

    def next_weights(f):
        for copy in weight_copies(f):
            copy.wait()

        @pl.when(f + 1 < 4 * n)
        def _():
            for copy in weight_copies(f + 1):
                copy.start()

        return lax.rem(f, 2)

    def to_across(src, dst, k):
        return pltpu.make_async_remote_copy(
            src_ref=src, dst_ref=dst, send_sem=far_send.at[k], recv_sem=far_recv.at[k], device_id={"dp": across}, device_id_type=MESH)

    for copy in weight_copies(0):
        copy.start()
    get_x = pltpu.make_async_copy(x_hbm, h, x_sem.at[0])
    get_x.start()
    get_dy = pltpu.make_async_copy(dy_hbm, dh, x_sem.at[1])
    get_dy.start()
    barrier = pltpu.get_barrier_semaphore()
    for other in (partner, across):
        pl.semaphore_signal(barrier, inc=1, device_id={"dp": other}, device_id_type=MESH)
    pl.semaphore_wait(barrier, 2)
    send_dy = to_across(dy_hbm, far_dy, 0)
    send_dy.start()
    ssv[...] = jnp.zeros_like(ssv)
    get_x.wait()

    def first_norm(r, _):
        wide = h[rows(r), :].astype(F32)
        a[rows(r), :] = (wide * norm_scale(wide)).astype(BF16)
        acc[rows(r), :] = jnp.zeros((ROWS, d), F32)
        return 0

    lax.fori_loop(0, blocks, first_norm, 0)

    def forward(j, _):
        slot = next_weights(j)
        for r in range(blocks):
            here = pl.ds(r * ROWS, ROWS)
            both = dot(a[here, :], wgu[slot])
            gate, up = both[:, :J], both[:, J:]
            acc[here, :] += dot((gate * jax.nn.sigmoid(gate) * up).astype(BF16), wd[slot])
        return 0

    lax.fori_loop(0, n, forward, 0)

    def end_layer_0(r, _):
        h[rows(r), :] = h[rows(r), :] + acc[rows(r), :].astype(BF16)
        acc[rows(r), :] = jnp.zeros((ROWS, d), F32)
        return 0

    lax.fori_loop(0, blocks, end_layer_0, 0)
    keep_h = pltpu.make_async_copy(h, h_hbm, x_sem.at[0])
    keep_h.start()
    get_dy.wait()
    keep_h.wait()
    send_h = to_across(h_hbm, far_h, 1)
    send_h.start()

    def to_layer_0(r, _):
        by_a = acc[rows(r), :].astype(BF16).astype(F32)
        wide = h[rows(r), :].astype(F32)
        mean = jnp.mean(wide**2, -1, keepdims=True) + 1e-6
        scale = lax.rsqrt(mean)
        by_scale = jnp.sum(by_a * wide, -1, keepdims=True)
        by_wide = by_a * scale - wide * (by_scale * scale / mean * (1.0 / d))
        dh[rows(r), :] = (dh[rows(r), :].astype(F32) + by_wide.astype(BF16).astype(F32)).astype(BF16)
        return 0

    def begin(r, _):
        wide = h[rows(r), :].astype(F32)
        a[rows(r), :] = (wide * norm_scale(wide)).astype(BF16)
        at[:, rows(r)] = a[rows(r), :].T
        dht[:, rows(r)] = dh[rows(r), :].T
        return 0

    def s1(u):
        slot = lax.rem(u, 2)
        return pltpu.make_async_remote_copy(
            src_ref=grad.at[:, half_of(1 - core), :], dst_ref=near.at[slot],
            send_sem=s1_send, recv_sem=s1_recv.at[slot], device_id={"dp": partner}, device_id_type=MESH)

    def s2(j):
        return pltpu.make_async_remote_copy(
            src_ref=chip.at[j], dst_ref=far.at[j], send_sem=s2_send.at[j], recv_sem=s2_recv.at[j],
            device_id={"dp": across}, device_id_type=MESH)

    def places(layer, j):
        slot, index = 2 * layer + lax.rem(j, 2), layer * n + j
        return [
            (total.at[slot], g_hbm.at[index, :, half_of(core), :], slot, index),
            (total_d.at[slot], gd_hbm.at[index, :, half_of(core)], 4 + slot, 2 * n + index),
        ]

    def s3(layer, j):
        return [
            pltpu.make_async_remote_copy(
                src_ref=src, dst_ref=dst, send_sem=s3_send.at[slot], recv_sem=s3_recv.at[index], device_id={"dp": partner}, device_id_type=MESH)
            for src, dst, slot, index in places(layer, j)
        ]

    def put(layer, j):
        return [pltpu.make_async_copy(src, dst, put_sem.at[slot]) for src, dst, slot, _ in places(layer, j)]

    def drained(layer, j):
        for copy in s3(layer, j):
            copy.wait_send()
        for copy in put(layer, j):
            copy.wait()

    def leave(layer, j):
        for copy in s3(layer, j) + put(layer, j):
            copy.start()

    def free_total(layer, j):
        @pl.when(j >= 2)
        def _():
            drained(layer, j - 2)

    def deliver(layer, j, new, k):
        wide = new.astype(F32)
        if k == 2:
            total_d[2 * layer + lax.rem(j, 2)] = wide.T.astype(BF16)
        else:
            total[2 * layer + lax.rem(j, 2), k] = new
        ssv[...] += jnp.sum((wide * wide).reshape(half // 8, 8, J), 0)

    def keep(j):
        return pltpu.make_async_copy(grad, own_hbm.at[j], own_sem)

    most, left, right = pl.ds(0, tokens), pl.ds(0, d), pl.ds(d, d)
    hand = {
        "acc": [(md_hbm.at[0, most, :], acc)],
        "h": [(wd_hbm.at[1, most, :], h)],
        "a": [(wd_hbm.at[0, most, :], a)],
        "dh": [(wg_hbm.at[1, :, left], dh.at[left, :]), (wg_hbm.at[1, :, right], dh.at[right, :])],
        "at": [(wg_hbm.at[0, :, most], at)],
        "dht": [(wu_hbm.at[0, :, most], dht)],
    }
    hand = {name: [(*pair, k) for pair in pairs] for k, (name, pairs) in enumerate(hand.items())}
    hand["dh"][1] = (*hand["dh"][1][:2], len(hand))

    def handed(*names):
        return [pltpu.make_async_copy(src, dst, hand_sem.at[k]) for name in names for src, dst, k in hand[name]]

    def step(t, _):
        p, j = t // n, lax.rem(t, n)

        @pl.when(jnp.logical_and(p == 1, j == 0))
        def _():
            keep(n - 1).wait()
            lax.fori_loop(0, blocks, to_layer_0, 0)
            get = pltpu.make_async_copy(x_hbm, h, x_sem.at[0])
            get.start()
            get.wait()

        @pl.when(jnp.logical_and(p == 2, j == 0))
        def _():
            to_across(dy_hbm, far_dy, 0).wait()
            to_across(h_hbm, far_h, 1).wait()
            get = pltpu.make_async_copy(far_h, h, x_sem.at[0])
            get.start()
            get_too = pltpu.make_async_copy(far_dy, dh, x_sem.at[1])
            get_too.start()
            get.wait()
            get_too.wait()

        @pl.when(j == 0)
        def _():
            lax.fori_loop(0, blocks, begin, 0)

        @pl.when(jnp.logical_and(p == 2, j == 0))
        def _():
            for copy in handed("acc", "h"):
                copy.start()

        slot = next_weights(n + t)

        @pl.when(p == 2)
        def _():
            pltpu.make_async_copy(own_hbm.at[j], mine, own_sem).start()

        def block(r, _):
            here = rows(r)
            both = dot(a[here, :], wgu[slot])
            gate, up = both[:, :J], both[:, J:]
            by_act = dot_nt(dh[here, :], wd[slot]).astype(BF16).astype(F32)
            s = jax.nn.sigmoid(gate)
            silu = gate * s
            act[here, :] = (silu * up).astype(BF16)
            dgu[here, J:] = (by_act * silu).astype(BF16)
            dgu[here, :J] = (by_act * up * (s + silu * (1.0 - s))).astype(BF16)
            return 0

        lax.fori_loop(0, blocks, block, 0, unroll=True)

        @pl.when(t == 3 * n - 1)
        def _():
            for copy in handed("a", "dh"):
                copy.start()

        @pl.when(jnp.logical_and(p == 0, j > 0))
        def _():
            keep(j - 1).wait()

        def rest(i, _):
            here = half_of(lax.rem(1 - core + i, 2))
            both = dot(at[here, :], dgu[...]).astype(BF16)
            grad[0, here, :] = both[:, :J]
            grad[1, here, :] = both[:, J:]
            grad[2, here, :] = dot(dht[here, :], act[...]).astype(BF16)

            @pl.when(jnp.logical_and(i == 0, p == 2))
            def _():
                pltpu.make_async_copy(own_hbm.at[j], mine, own_sem).wait()
                for k in range(3):
                    grad[k, here, :] = (grad[k, here, :].astype(F32) + mine[k, here, :].astype(F32)).astype(BF16)

            @pl.when(jnp.logical_and(i == 0, p >= 1))
            def _():
                s1(t - n).start()

            return 0

        lax.fori_loop(0, 2, rest, 0)

        @pl.when(t == 3 * n - 1)
        def _():
            for copy in handed("at", "dht"):
                copy.start()

        @pl.when(p == 0)
        def _():
            keep(j).start()

            def back(r, _):
                acc[rows(r), :] += dot_nt(dgu[rows(r), :], wgu[slot])
                return 0

            lax.fori_loop(0, blocks, back, 0, unroll=True)

        @pl.when(p == 1)
        def _():
            s1(t - n).wait()
            for k in range(3):
                chip[j, k] = (grad[k, half_of(core), :].astype(F32) + near[lax.rem(t - n, 2), k].astype(F32)).astype(BF16)
            s2(j).start()

        @pl.when(p == 2)
        def _():
            free_total(1, j)
            s1(t - n).wait()
            for k in range(3):
                new = grad[k, half_of(core), :].astype(F32) + mine[k, half_of(core), :].astype(F32)
                deliver(1, j, (new + near[lax.rem(t - n, 2), k].astype(F32)).astype(BF16), k)
            leave(1, j)
            free_total(0, j)
            s2(j).wait()
            for k in range(3):
                deliver(0, j, (chip[j, k].astype(F32) + far[j, k].astype(F32)).astype(BF16), k)
            leave(0, j)

        return 0

    lax.fori_loop(0, 3 * n, step, 0)
    share = pltpu.make_async_remote_copy(
        src_ref=ssv, dst_ref=ssr, send_sem=ss_sem.at[0], recv_sem=ss_sem.at[1], device_id={"dp": partner}, device_id_type=MESH)
    share.start()
    for layer in range(2):
        for j in (n - 2, n - 1):
            drained(layer, j)

    def arrived(j, _):
        for copy in s3(0, j) + s3(1, j):
            copy.wait_recv()
        return 0

    lax.fori_loop(0, n, arrived, 0)
    share.wait()
    for copy in handed(*hand):
        copy.wait()
    ss_ref[...] = ssv[...] + ssr[...]


def call_gradients(x, dy, wg, wu, wd, md):
    tokens, d = x.shape
    n = wg.shape[2] // J
    half = d // 2
    hbm = pl.BlockSpec(memory_space=pltpu.HBM)
    vmem = pl.BlockSpec(memory_space=pltpu.VMEM)
    dma = pltpu.SemaphoreType.DMA
    part = (3, half, J)
    operands = [pltpu.with_memory_space_constraint(one, pltpu.HBM) for one in (x, dy, wg, wu, wd, md)]
    g, gd, ss, _, _, _, _, *kept = pl.pallas_call(
        gradients,
        name="gradients",
        out_shape=(
            pltpu.HBM((2 * n, 2, d, J), BF16), pltpu.HBM((2 * n, J, d), BF16), jax.ShapeDtypeStruct((8, J), F32),
            *[pltpu.HBM((tokens, d), BF16)] * 3, pltpu.HBM((n, 3, d, J), BF16),
            pltpu.VMEM((tokens, d), BF16), pltpu.VMEM((tokens, d), BF16), pltpu.VMEM((d, tokens), BF16),
            pltpu.VMEM((tokens, d), BF16), pltpu.VMEM((d, tokens), BF16), pltpu.VMEM((tokens, d), F32),
        ),
        in_specs=[hbm] * 6,
        out_specs=(hbm, hbm, vmem, hbm, hbm, hbm, hbm, *[vmem] * 6),
        scratch_shapes=[
            pltpu.VMEM((tokens, J), BF16), pltpu.VMEM((tokens, 2 * J), BF16),
            pltpu.VMEM((2, d, 2 * J), BF16), pltpu.VMEM((2, J, d), BF16),
            pltpu.VMEM((3, d, J), BF16), pltpu.VMEM((3, d, J), BF16), pltpu.VMEM((2, *part), BF16), pltpu.VMEM((n, *part), BF16),
            pltpu.VMEM((n, *part), BF16), pltpu.VMEM((4, 2, half, J), BF16), pltpu.VMEM((4, J, half), BF16),
            pltpu.VMEM((8, J), F32), pltpu.VMEM((8, J), F32),
            dma((3, 2)), dma((2,)), dma, dma((2,)), dma((2,)), dma, dma((2,)), dma((n,)), dma((n,)), dma((8,)), dma((4 * n,)), dma((8,)), dma((2,)), dma((7,)),
        ],
        compiler_params=pltpu.CompilerParams(collective_id=0, has_side_effects=True, vmem_limit_bytes=VMEM_LIMIT - HANDED),
    )(*operands)
    return (g, gd), ss, kept


def adamw(count, near, ss, h, a, at, dh, dht, acc, g, gd, wg, wu, wd, mg, mu, md, vg, vu, vd, *outs):
    d = wg.shape[1]
    layer, j = pl.program_id(0), pl.program_id(1)
    here = jnp.minimum(j, near - 1)
    chunk = pl.ds(pl.multiple_of(here * J, J), J)
    kept, first = j < near, layer == 0
    squares = jnp.sum(jnp.sum(ss[...], 0, keepdims=True), 1, keepdims=True)
    factor = jnp.minimum(1.0, 0.5 * lax.rsqrt(squares / count + 1e-30))

    def take(k, size, w, m, v):
        def some(i, _):
            piece = pl.ds(pl.multiple_of(i * size, size), size)
            mine = (gd[0, piece, :] if k == 2 else g[0, k, piece, :]).astype(F32) * factor
            new_m = 0.9 * m(piece) + 0.1 * mine
            new_v = 0.95 * v(piece) + 0.05 * mine * mine
            old = w(piece).astype(F32)
            outs[k][0, piece, :] = (old - 0.02 * (new_m * lax.rsqrt(new_v + 1e-8) + 0.1 * old)).astype(BF16)
            outs[3 + k][0, piece, :] = new_m
            outs[6 + k][0, piece, :] = new_v
            return 0

        lax.fori_loop(0, outs[k].shape[1] // size, some, 0, unroll=2)

    def rows_of(ref):
        return lambda piece: ref[0, piece, :]

    def of_chunk(ref):
        return lambda piece: ref[pl.ds(pl.multiple_of(here * J + piece.start, TALL), TALL), :]

    gate, up, down = (rows_of(mg), rows_of(vg)), (rows_of(mu), rows_of(vu)), (rows_of(md), rows_of(vd))

    @pl.when(jnp.logical_and(kept, first))
    def _():
        take(0, WIDE, lambda piece: at[piece, chunk], *gate)
        take(1, WIDE, lambda piece: dht[piece, chunk], *up)
        take(2, TALL, of_chunk(a), of_chunk(acc), down[1])

    @pl.when(jnp.logical_and(kept, layer == 1))
    def _():
        across = d // J
        cols = pl.ds(pl.multiple_of(here % across * J, J), J)
        take(0, WIDE, lambda piece: dh[pl.ds(pl.multiple_of(here // across * d + piece.start, WIDE), WIDE), cols], *gate)
        take(1, WIDE, rows_of(wu), *up)
        take(2, TALL, of_chunk(h), *down)

    @pl.when(j >= near)
    def _():
        take(0, WIDE, rows_of(wg), *gate)
        take(1, WIDE, rows_of(wu), *up)
        take(2, TALL, rows_of(wd), *down)


def call_adamw(ss, kept, g, weights, m, v):
    layers, d, ff = weights[0].shape
    n = ff // J
    near = kept[0].shape[0] // J
    vmem = pl.BlockSpec(memory_space=pltpu.VMEM)

    def there(l, j):
        return jnp.maximum(j, near)

    def there_0(l, j):
        return jnp.where(l == 0, jnp.maximum(j, near), j)

    def own(l, j):
        return j

    def wide(at):
        return pl.BlockSpec((1, d, J), lambda l, j: (l, 0, at(l, j)))

    def tall(at):
        return pl.BlockSpec((1, J, d), lambda l, j: (l, at(l, j), 0))

    count = float(3 * layers * d * ff)
    three = [wide(own), wide(own), tall(own)]
    kept = [pltpu.with_memory_space_constraint(one, pltpu.VMEM) for one in kept]
    return pl.pallas_call(
        lambda *refs: adamw(count, near, *refs),
        name="adamw",
        grid=(layers, n),
        out_shape=[jax.ShapeDtypeStruct(w.shape, t) for t in (BF16, F32, F32) for w in weights],
        in_specs=[pl.BlockSpec((8, J), lambda l, j: (0, 0)), *[vmem] * 6, pl.BlockSpec((1, 2, d, J), lambda l, j: (l * n + j, 0, 0, 0)),
                  pl.BlockSpec((1, J, d), lambda l, j: (l * n + j, 0, 0)),
                  wide(there), wide(there_0), tall(there), wide(own), wide(own), tall(there_0), *three],
        out_specs=three * 3,
        compiler_params=pltpu.CompilerParams(vmem_limit_bytes=VMEM_LIMIT - HANDED),
    )(ss, *kept, *g, *weights, *m, *v)


def solution(mesh):
    def step(x, dy, *arrays):
        weights, m, v = (arrays[i : i + 3] for i in (0, 3, 6))
        g, ss, kept = call_gradients(x[0], dy[0], *weights, m[2])
        return tuple(call_adamw(ss, kept, g, weights, m, v))

    return jax.shard_map(
        step,
        mesh=mesh,
        in_specs=(P(("rep", "dp"), None, None),) * 2 + (P(None, None, None),) * 9,
        out_specs=(P("rep", None, None),) * 9,
        check_vma=False,
    )
```

```python
import jax
import jax.numpy as jnp
from jax import lax
from jax.experimental import pallas as pl
from jax.experimental.pallas import tpu as pltpu
from jax.sharding import PartitionSpec as P

F32, BF16 = jnp.float32, jnp.bfloat16
J = 256
ROWS = 512
VMEM_LIMIT = 67043328
WIDE, TALL = 256, 64
HANDED = 28 * 2**20
MESH = pl.DeviceIdType.MESH


def dot(a, b):
    return jnp.dot(a, b, preferred_element_type=F32)


def dot_nt(a, b):
    return lax.dot_general(a, b, (((1,), (1,)), ((), ())), preferred_element_type=F32)


def norm_scale(wide):
    return lax.rsqrt(jnp.mean(wide**2, -1, keepdims=True) + 1e-6)


def gradients(x_hbm, dy_hbm, wg_hbm, wu_hbm, wd_hbm, md_hbm, g_hbm, gd_hbm, ss_ref, h_hbm, far_h, far_dy, own_hbm, h, a, at, dh, dht, acc, act, dgu, wgu, wd,
              grad, mine, near, chip, far, total, total_d, ssv, ssr, w_sem, x_sem, own_sem, far_send, far_recv, s1_send, s1_recv, s2_send, s2_recv,
              s3_send, s3_recv, put_sem, ss_sem, hand_sem):
    tokens, d = h.shape
    blocks = tokens // ROWS
    n = wg_hbm.shape[2] // J
    half = d // 2
    me = lax.axis_index("dp")
    core = lax.rem(me, 2)
    partner = me + 1 - 2 * core
    across = lax.rem(me + 2, 4)

    def rows(r):
        return pl.ds(pl.multiple_of(r * ROWS, ROWS), ROWS)

    def half_of(which):
        return pl.ds(pl.multiple_of(which * half, half), half)

    def weight_copies(f):
        slot, layer, j = lax.rem(f, 2), lax.rem(f // n, 2), lax.rem(f, n)
        cols = pl.ds(pl.multiple_of(j * J, J), J)
        return [
            pltpu.make_async_copy(wg_hbm.at[layer, :, cols], wgu.at[slot, :, pl.ds(0, J)], w_sem.at[0, slot]),
            pltpu.make_async_copy(wu_hbm.at[layer, :, cols], wgu.at[slot, :, pl.ds(J, J)], w_sem.at[1, slot]),
            pltpu.make_async_copy(wd_hbm.at[layer, cols, :], wd.at[slot], w_sem.at[2, slot]),
        ]

    def next_weights(f):
        for copy in weight_copies(f):
            copy.wait()

        @pl.when(f + 1 < 4 * n)
        def _():
            for copy in weight_copies(f + 1):
                copy.start()

        return lax.rem(f, 2)

    def to_across(src, dst, k):
        return pltpu.make_async_remote_copy(
            src_ref=src, dst_ref=dst, send_sem=far_send.at[k], recv_sem=far_recv.at[k], device_id={"dp": across}, device_id_type=MESH)

    for copy in weight_copies(0):
        copy.start()
    get_x = pltpu.make_async_copy(x_hbm, h, x_sem.at[0])
    get_x.start()
    get_dy = pltpu.make_async_copy(dy_hbm, dh, x_sem.at[1])
    get_dy.start()
    barrier = pltpu.get_barrier_semaphore()
    for other in (partner, across):
        pl.semaphore_signal(barrier, inc=1, device_id={"dp": other}, device_id_type=MESH)
    pl.semaphore_wait(barrier, 2)
    send_dy = to_across(dy_hbm, far_dy, 0)
    send_dy.start()
    ssv[...] = jnp.zeros_like(ssv)
    get_x.wait()

    def first_norm(r, _):
        wide = h[rows(r), :].astype(F32)
        a[rows(r), :] = (wide * norm_scale(wide)).astype(BF16)
        acc[rows(r), :] = jnp.zeros((ROWS, d), F32)
        return 0

    lax.fori_loop(0, blocks, first_norm, 0)

    def forward(j, _):
        slot = next_weights(j)
        for r in range(blocks):
            here = pl.ds(r * ROWS, ROWS)
            both = dot(a[here, :], wgu[slot])
            gate, up = both[:, :J], both[:, J:]
            acc[here, :] += dot((gate * jax.nn.sigmoid(gate) * up).astype(BF16), wd[slot])
        return 0

    lax.fori_loop(0, n, forward, 0)

    def end_layer_0(r, _):
        h[rows(r), :] = h[rows(r), :] + acc[rows(r), :].astype(BF16)
        acc[rows(r), :] = jnp.zeros((ROWS, d), F32)
        return 0

    lax.fori_loop(0, blocks, end_layer_0, 0)
    keep_h = pltpu.make_async_copy(h, h_hbm, x_sem.at[0])
    keep_h.start()
    get_dy.wait()
    keep_h.wait()
    send_h = to_across(h_hbm, far_h, 1)
    send_h.start()

    def to_layer_0(r, _):
        by_a = acc[rows(r), :].astype(BF16).astype(F32)
        wide = h[rows(r), :].astype(F32)
        mean = jnp.mean(wide**2, -1, keepdims=True) + 1e-6
        scale = lax.rsqrt(mean)
        by_scale = jnp.sum(by_a * wide, -1, keepdims=True)
        by_wide = by_a * scale - wide * (by_scale * scale / mean * (1.0 / d))
        dh[rows(r), :] = (dh[rows(r), :].astype(F32) + by_wide.astype(BF16).astype(F32)).astype(BF16)
        return 0

    def begin(r, _):
        wide = h[rows(r), :].astype(F32)
        a[rows(r), :] = (wide * norm_scale(wide)).astype(BF16)
        at[:, rows(r)] = a[rows(r), :].T
        dht[:, rows(r)] = dh[rows(r), :].T
        return 0

    def s1(u):
        slot = lax.rem(u, 2)
        return pltpu.make_async_remote_copy(
            src_ref=grad.at[:, half_of(1 - core), :], dst_ref=near.at[slot],
            send_sem=s1_send, recv_sem=s1_recv.at[slot], device_id={"dp": partner}, device_id_type=MESH)

    def s2(j, k):
        return pltpu.make_async_remote_copy(
            src_ref=chip.at[j, k], dst_ref=far.at[j, k], send_sem=s2_send.at[j, k], recv_sem=s2_recv.at[j, k],
            device_id={"dp": across}, device_id_type=MESH)

    def places(layer, j):
        slot, index = 2 * layer + lax.rem(j, 2), layer * n + j
        return [
            (total.at[slot], g_hbm.at[index, :, half_of(core), :], slot, index),
            (total_d.at[slot], gd_hbm.at[index, :, half_of(core)], 4 + slot, 2 * n + index),
        ]

    def s3(layer, j):
        return [
            pltpu.make_async_remote_copy(
                src_ref=src, dst_ref=dst, send_sem=s3_send.at[slot], recv_sem=s3_recv.at[index], device_id={"dp": partner}, device_id_type=MESH)
            for src, dst, slot, index in places(layer, j)
        ]

    def put(layer, j):
        return [pltpu.make_async_copy(src, dst, put_sem.at[slot]) for src, dst, slot, _ in places(layer, j)]

    def drained(layer, j):
        for copy in s3(layer, j):
            copy.wait_send()
        for copy in put(layer, j):
            copy.wait()

    def leave(layer, j, k):
        if k > 0:
            s3(layer, j)[k - 1].start()
            put(layer, j)[k - 1].start()

    def free_total(layer, j):
        @pl.when(j >= 2)
        def _():
            drained(layer, j - 2)

    def deliver(layer, j, new, k):
        wide = new.astype(F32)
        if k == 2:
            total_d[2 * layer + lax.rem(j, 2)] = wide.T.astype(BF16)
        else:
            total[2 * layer + lax.rem(j, 2), k] = new
        ssv[...] += jnp.sum((wide * wide).reshape(half // 8, 8, J), 0)

    def keep(j):
        return pltpu.make_async_copy(grad, own_hbm.at[j], own_sem)

    most, left, right = pl.ds(0, tokens), pl.ds(0, d), pl.ds(d, d)
    hand = {
        "acc": [(md_hbm.at[1, most, :], acc)],
        "h": [(wd_hbm.at[1, most, :], h)],
        "a": [(wd_hbm.at[0, most, :], a)],
        "dh": [(wg_hbm.at[1, :, left], dh.at[left, :]), (wg_hbm.at[1, :, right], dh.at[right, :])],
        "at": [(wg_hbm.at[0, :, most], at)],
        "dht": [(wu_hbm.at[0, :, most], dht)],
    }
    hand = {name: [(*pair, k) for pair in pairs] for k, (name, pairs) in enumerate(hand.items())}
    hand["dh"][1] = (*hand["dh"][1][:2], len(hand))

    def handed(*names):
        return [pltpu.make_async_copy(src, dst, hand_sem.at[k]) for name in names for src, dst, k in hand[name]]

    def step(t, _):
        p, j = t // n, lax.rem(t, n)

        @pl.when(jnp.logical_and(p == 1, j == 0))
        def _():
            keep(n - 1).wait()
            lax.fori_loop(0, blocks, to_layer_0, 0)
            get = pltpu.make_async_copy(x_hbm, h, x_sem.at[0])
            get.start()
            get.wait()

        @pl.when(jnp.logical_and(p == 2, j == 0))
        def _():
            to_across(dy_hbm, far_dy, 0).wait()
            to_across(h_hbm, far_h, 1).wait()
            get = pltpu.make_async_copy(far_h, h, x_sem.at[0])
            get.start()
            get_too = pltpu.make_async_copy(far_dy, dh, x_sem.at[1])
            get_too.start()
            get.wait()
            get_too.wait()

        @pl.when(j == 0)
        def _():
            lax.fori_loop(0, blocks, begin, 0)

        @pl.when(jnp.logical_and(p == 2, j == 0))
        def _():
            for copy in handed("acc", "h"):
                copy.start()

        slot = next_weights(n + t)

        @pl.when(p == 2)
        def _():
            pltpu.make_async_copy(own_hbm.at[j], mine, own_sem).start()

        def block(r, _):
            here = rows(r)
            both = dot(a[here, :], wgu[slot])
            gate, up = both[:, :J], both[:, J:]
            by_act = dot_nt(dh[here, :], wd[slot]).astype(BF16).astype(F32)
            s = jax.nn.sigmoid(gate)
            silu = gate * s
            act[here, :] = (silu * up).astype(BF16)
            dgu[here, J:] = (by_act * silu).astype(BF16)
            dgu[here, :J] = (by_act * up * (s + silu * (1.0 - s))).astype(BF16)
            return 0

        lax.fori_loop(0, blocks, block, 0, unroll=True)

        @pl.when(t == 3 * n - 1)
        def _():
            for copy in handed("a", "dh"):
                copy.start()

        @pl.when(jnp.logical_and(p == 0, j > 0))
        def _():
            keep(j - 1).wait()

        def rest(i, _):
            here = half_of(lax.rem(1 - core + i, 2))
            both = dot(at[here, :], dgu[...]).astype(BF16)
            grad[0, here, :] = both[:, :J]
            grad[1, here, :] = both[:, J:]
            grad[2, here, :] = dot(dht[here, :], act[...]).astype(BF16)

            @pl.when(jnp.logical_and(i == 0, p == 2))
            def _():
                pltpu.make_async_copy(own_hbm.at[j], mine, own_sem).wait()
                for k in range(3):
                    grad[k, here, :] = (grad[k, here, :].astype(F32) + mine[k, here, :].astype(F32)).astype(BF16)

            @pl.when(jnp.logical_and(i == 0, p >= 1))
            def _():
                s1(t - n).start()

            return 0

        lax.fori_loop(0, 2, rest, 0)

        @pl.when(t == 3 * n - 1)
        def _():
            for copy in handed("at", "dht"):
                copy.start()

        @pl.when(p == 0)
        def _():
            keep(j).start()

            def back(r, _):
                acc[rows(r), :] += dot_nt(dgu[rows(r), :], wgu[slot])
                return 0

            lax.fori_loop(0, blocks, back, 0, unroll=True)

        @pl.when(p == 1)
        def _():
            s1(t - n).wait()
            for k in range(3):
                chip[j, k] = (grad[k, half_of(core), :].astype(F32) + near[lax.rem(t - n, 2), k].astype(F32)).astype(BF16)
                s2(j, k).start()

        @pl.when(p == 2)
        def _():
            free_total(1, j)
            s1(t - n).wait()
            for k in range(3):
                new = grad[k, half_of(core), :].astype(F32) + mine[k, half_of(core), :].astype(F32)
                deliver(1, j, (new + near[lax.rem(t - n, 2), k].astype(F32)).astype(BF16), k)
                leave(1, j, k)
            free_total(0, j)
            for k in range(3):
                s2(j, k).wait()
                deliver(0, j, (chip[j, k].astype(F32) + far[j, k].astype(F32)).astype(BF16), k)
                leave(0, j, k)

        return 0

    lax.fori_loop(0, 3 * n, step, 0)
    share = pltpu.make_async_remote_copy(
        src_ref=ssv, dst_ref=ssr, send_sem=ss_sem.at[0], recv_sem=ss_sem.at[1], device_id={"dp": partner}, device_id_type=MESH)
    share.start()
    for layer in range(2):
        for j in (n - 2, n - 1):
            drained(layer, j)

    def arrived(j, _):
        for copy in s3(0, j) + s3(1, j):
            copy.wait_recv()
        return 0

    lax.fori_loop(0, n, arrived, 0)
    share.wait()
    for copy in handed(*hand):
        copy.wait()
    ss_ref[...] = ssv[...] + ssr[...]


def call_gradients(x, dy, wg, wu, wd, md):
    tokens, d = x.shape
    n = wg.shape[2] // J
    half = d // 2
    hbm = pl.BlockSpec(memory_space=pltpu.HBM)
    vmem = pl.BlockSpec(memory_space=pltpu.VMEM)
    dma = pltpu.SemaphoreType.DMA
    part = (3, half, J)
    operands = [pltpu.with_memory_space_constraint(one, pltpu.HBM) for one in (x, dy, wg, wu, wd, md)]
    g, gd, ss, _, _, _, _, *kept = pl.pallas_call(
        gradients,
        name="gradients",
        out_shape=(
            pltpu.HBM((2 * n, 2, d, J), BF16), pltpu.HBM((2 * n, J, d), BF16), jax.ShapeDtypeStruct((8, J), F32),
            *[pltpu.HBM((tokens, d), BF16)] * 3, pltpu.HBM((n, 3, d, J), BF16),
            pltpu.VMEM((tokens, d), BF16), pltpu.VMEM((tokens, d), BF16), pltpu.VMEM((d, tokens), BF16),
            pltpu.VMEM((tokens, d), BF16), pltpu.VMEM((d, tokens), BF16), pltpu.VMEM((tokens, d), F32),
        ),
        in_specs=[hbm] * 6,
        out_specs=(hbm, hbm, vmem, hbm, hbm, hbm, hbm, *[vmem] * 6),
        scratch_shapes=[
            pltpu.VMEM((tokens, J), BF16), pltpu.VMEM((tokens, 2 * J), BF16),
            pltpu.VMEM((2, d, 2 * J), BF16), pltpu.VMEM((2, J, d), BF16),
            pltpu.VMEM((3, d, J), BF16), pltpu.VMEM((3, d, J), BF16), pltpu.VMEM((2, *part), BF16), pltpu.VMEM((n, *part), BF16),
            pltpu.VMEM((n, *part), BF16), pltpu.VMEM((4, 2, half, J), BF16), pltpu.VMEM((4, J, half), BF16),
            pltpu.VMEM((8, J), F32), pltpu.VMEM((8, J), F32),
            dma((3, 2)), dma((2,)), dma, dma((2,)), dma((2,)), dma, dma((2,)), dma((n, 3)), dma((n, 3)), dma((8,)), dma((4 * n,)), dma((8,)), dma((2,)), dma((7,)),
        ],
        compiler_params=pltpu.CompilerParams(collective_id=0, has_side_effects=True, vmem_limit_bytes=VMEM_LIMIT - HANDED),
    )(*operands)
    return (g, gd), ss, kept


def adamw(count, near, ss, h, a, at, dh, dht, acc, g, gd, wg, wu, wd, mg, mu, md, vg, vu, vd, *outs):
    d = 2 * wg.shape[1]
    row, row_d = pl.program_id(2) * wg.shape[1], pl.program_id(2) * wd.shape[1]
    layer, j = pl.program_id(0), pl.program_id(1)
    here = jnp.minimum(j, near - 1)
    chunk = pl.ds(pl.multiple_of(here * J, J), J)
    kept, first = j < near, layer == 0
    squares = jnp.sum(jnp.sum(ss[...], 0, keepdims=True), 1, keepdims=True)
    factor = jnp.minimum(1.0, 0.5 * lax.rsqrt(squares / count + 1e-30))

    def take(k, size, w, m, v):
        def some(i, _):
            piece = pl.ds(pl.multiple_of(i * size, size), size)
            mine = (gd[0, piece, :] if k == 2 else g[0, k, piece, :]).astype(F32) * factor
            new_m = 0.9 * m(piece) + 0.1 * mine
            new_v = 0.95 * v(piece) + 0.05 * mine * mine
            old = w(piece).astype(F32)
            outs[k][0, piece, :] = (old - 0.02 * (new_m * lax.rsqrt(new_v + 1e-8) + 0.1 * old)).astype(BF16)
            outs[3 + k][0, piece, :] = new_m
            outs[6 + k][0, piece, :] = new_v
            return 0

        lax.fori_loop(0, outs[k].shape[1] // size, some, 0, unroll=2)

    def rows_of(ref):
        return lambda piece: ref[0, piece, :]

    def rows(piece):
        return pl.ds(pl.multiple_of(row + piece.start, WIDE), WIDE)

    def of_chunk(ref):
        return lambda piece: ref[pl.ds(pl.multiple_of(here * J + row_d + piece.start, TALL), TALL), :]

    gate, up, down = (rows_of(mg), rows_of(vg)), (rows_of(mu), rows_of(vu)), (rows_of(md), rows_of(vd))

    @pl.when(jnp.logical_and(kept, first))
    def _():
        take(0, WIDE, lambda piece: at[rows(piece), chunk], *gate)
        take(1, WIDE, lambda piece: dht[rows(piece), chunk], *up)
        take(2, TALL, of_chunk(a), *down)

    @pl.when(jnp.logical_and(kept, layer == 1))
    def _():
        across = d // J
        cols = pl.ds(pl.multiple_of(here % across * J, J), J)
        take(0, WIDE, lambda piece: dh[pl.ds(pl.multiple_of(here // across * d + row + piece.start, WIDE), WIDE), cols], *gate)
        take(1, WIDE, rows_of(wu), *up)
        take(2, TALL, of_chunk(h), of_chunk(acc), down[1])

    @pl.when(j >= near)
    def _():
        take(0, WIDE, rows_of(wg), *gate)
        take(1, WIDE, rows_of(wu), *up)
        take(2, TALL, rows_of(wd), *down)


def call_adamw(ss, kept, g, weights, m, v):
    layers, d, ff = weights[0].shape
    n = ff // J
    near = kept[0].shape[0] // J
    vmem = pl.BlockSpec(memory_space=pltpu.VMEM)

    def there(l, j):
        return jnp.maximum(j, near)

    def there_0(l, j):
        return jnp.where(l == 0, jnp.maximum(j, near), j)

    def there_1(l, j):
        return jnp.where(l == 1, jnp.maximum(j, near), j)

    def own(l, j):
        return j

    def wide(at, mode=None):
        return pl.BlockSpec((1, d // 2, J), lambda l, j, i: (l, jnp.where(at(l, j) == j, i, 0), at(l, j)), pipeline_mode=mode)

    def tall(at, mode=None):
        return pl.BlockSpec((1, J // 2, d), lambda l, j, i: (l, 2 * at(l, j) + jnp.where(at(l, j) == j, i, 0), 0), pipeline_mode=mode)

    count = float(3 * layers * d * ff)
    mode, mode_out = pl.Buffered(4), pl.Buffered(2)
    kept = [pltpu.with_memory_space_constraint(one, pltpu.VMEM) for one in kept]
    gs = [pl.BlockSpec((1, 2, d // 2, J), lambda l, j, i: (l * n + j, 0, i, 0), pipeline_mode=mode),
          pl.BlockSpec((1, J // 2, d), lambda l, j, i: (l * n + j, i, 0), pipeline_mode=mode)]
    hbm = pl.BlockSpec(memory_space=pltpu.HBM)

    def kernel(ss, h, a, at, dh, dht, acc, *refs):
        pltpu.emit_pipeline(
            lambda *blocks: adamw(count, near, ss, h, a, at, dh, dht, acc, *blocks),
            grid=(layers, n, 2),
            in_specs=[*gs, wide(there), wide(there_0), tall(there), wide(own, mode), wide(own, mode), tall(there_1, mode),
                      wide(own, mode), wide(own, mode), tall(own, mode)],
            out_specs=[wide(own, mode_out), wide(own, mode_out), tall(own, mode_out)] * 3,
        )(*refs)

    arrays = [pltpu.with_memory_space_constraint(one, pltpu.HBM) for one in (*g, *weights, *m, *v)]
    return pl.pallas_call(
        kernel,
        name="adamw",
        out_shape=[pltpu.HBM(w.shape, t) for t in (BF16, F32, F32) for w in weights],
        in_specs=[vmem] * 7 + [hbm] * len(arrays),
        out_specs=[hbm] * 9,
        compiler_params=pltpu.CompilerParams(vmem_limit_bytes=VMEM_LIMIT - HANDED),
    )(ss, *kept, *arrays)


def solution(mesh):
    def step(x, dy, *arrays):
        weights, m, v = (arrays[i : i + 3] for i in (0, 3, 6))
        g, ss, kept = call_gradients(x[0], dy[0], *weights, m[2])
        return tuple(call_adamw(ss, kept, g, weights, m, v))

    return jax.shard_map(
        step,
        mesh=mesh,
        in_specs=(P(("rep", "dp"), None, None),) * 2 + (P(None, None, None),) * 9,
        out_specs=(P("rep", None, None),) * 9,
        check_vma=False,
    )
```

```python
import jax
import jax.numpy as jnp
from jax import lax
from jax.experimental import pallas as pl
from jax.experimental.pallas import tpu as pltpu
from jax.sharding import PartitionSpec as P

F32, BF16 = jnp.float32, jnp.bfloat16
J = 256
ROWS = 512
VMEM_LIMIT = 67043328
WIDE, TALL = 256, 64
HANDED = 71 * 2**19
MESH = pl.DeviceIdType.MESH


def dot(a, b):
    return jnp.dot(a, b, preferred_element_type=F32)


def dot_nt(a, b):
    return lax.dot_general(a, b, (((1,), (1,)), ((), ())), preferred_element_type=F32)


def norm_scale(wide):
    return lax.rsqrt(jnp.mean(wide**2, -1, keepdims=True) + 1e-6)


def gradients(x_hbm, dy_hbm, wg_hbm, wu_hbm, wd_hbm, md_hbm, g_hbm, gd_hbm, ss_ref, h_hbm, far_h, far_dy, own_hbm, h, a, at, dh, dht, acc, chip, act, dgu, wgu, wd,
              grad, mine, near, far, total, total_d, ssv, ssr, w_sem, x_sem, own_sem, far_send, far_recv, s1_send, s1_recv, s2_send, s2_recv,
              s3_send, s3_recv, put_sem, ss_sem, hand_sem):
    tokens, d = h.shape
    blocks = tokens // ROWS
    n = wg_hbm.shape[2] // J
    half = d // 2
    me = lax.axis_index("dp")
    core = lax.rem(me, 2)
    partner = me + 1 - 2 * core
    across = lax.rem(me + 2, 4)

    def rows(r):
        return pl.ds(pl.multiple_of(r * ROWS, ROWS), ROWS)

    def half_of(which):
        return pl.ds(pl.multiple_of(which * half, half), half)

    def weight_copies(f):
        slot, layer, j = lax.rem(f, 2), lax.rem(f // n, 2), lax.rem(f, n)
        cols = pl.ds(pl.multiple_of(j * J, J), J)
        return [
            pltpu.make_async_copy(wg_hbm.at[layer, :, cols], wgu.at[slot, :, pl.ds(0, J)], w_sem.at[0, slot]),
            pltpu.make_async_copy(wu_hbm.at[layer, :, cols], wgu.at[slot, :, pl.ds(J, J)], w_sem.at[1, slot]),
            pltpu.make_async_copy(wd_hbm.at[layer, cols, :], wd.at[slot], w_sem.at[2, slot]),
        ]

    def next_weights(f):
        for copy in weight_copies(f):
            copy.wait()

        @pl.when(f + 1 < 4 * n)
        def _():
            for copy in weight_copies(f + 1):
                copy.start()

        return lax.rem(f, 2)

    def to_across(src, dst, k):
        return pltpu.make_async_remote_copy(
            src_ref=src, dst_ref=dst, send_sem=far_send.at[k], recv_sem=far_recv.at[k], device_id={"dp": across}, device_id_type=MESH)

    for copy in weight_copies(0):
        copy.start()
    get_x = pltpu.make_async_copy(x_hbm, h, x_sem.at[0])
    get_x.start()
    get_dy = pltpu.make_async_copy(dy_hbm, dh, x_sem.at[1])
    get_dy.start()
    barrier = pltpu.get_barrier_semaphore()
    for other in (partner, across):
        pl.semaphore_signal(barrier, inc=1, device_id={"dp": other}, device_id_type=MESH)
    pl.semaphore_wait(barrier, 2)
    send_dy = to_across(dy_hbm, far_dy, 0)
    send_dy.start()
    ssv[...] = jnp.zeros_like(ssv)
    get_x.wait()

    def first_norm(r, _):
        wide = h[rows(r), :].astype(F32)
        a[rows(r), :] = (wide * norm_scale(wide)).astype(BF16)
        acc[rows(r), :] = jnp.zeros((ROWS, d), F32)
        return 0

    lax.fori_loop(0, blocks, first_norm, 0)

    def forward(j, _):
        slot = next_weights(j)
        for r in range(blocks):
            here = pl.ds(r * ROWS, ROWS)
            both = dot(a[here, :], wgu[slot])
            gate, up = both[:, :J], both[:, J:]
            acc[here, :] += dot((gate * jax.nn.sigmoid(gate) * up).astype(BF16), wd[slot])
        return 0

    lax.fori_loop(0, n, forward, 0)

    def end_layer_0(r, _):
        h[rows(r), :] = h[rows(r), :] + acc[rows(r), :].astype(BF16)
        acc[rows(r), :] = jnp.zeros((ROWS, d), F32)
        return 0

    lax.fori_loop(0, blocks, end_layer_0, 0)
    keep_h = pltpu.make_async_copy(h, h_hbm, x_sem.at[0])
    keep_h.start()
    get_dy.wait()
    keep_h.wait()
    send_h = to_across(h_hbm, far_h, 1)
    send_h.start()

    def to_layer_0(r, _):
        by_a = acc[rows(r), :].astype(BF16).astype(F32)
        wide = h[rows(r), :].astype(F32)
        mean = jnp.mean(wide**2, -1, keepdims=True) + 1e-6
        scale = lax.rsqrt(mean)
        by_scale = jnp.sum(by_a * wide, -1, keepdims=True)
        by_wide = by_a * scale - wide * (by_scale * scale / mean * (1.0 / d))
        dh[rows(r), :] = (dh[rows(r), :].astype(F32) + by_wide.astype(BF16).astype(F32)).astype(BF16)
        return 0

    def begin(r, _):
        wide = h[rows(r), :].astype(F32)
        a[rows(r), :] = (wide * norm_scale(wide)).astype(BF16)
        at[:, rows(r)] = a[rows(r), :].T
        dht[:, rows(r)] = dh[rows(r), :].T
        return 0

    def s1(u):
        slot = lax.rem(u, 2)
        return pltpu.make_async_remote_copy(
            src_ref=grad.at[:, half_of(1 - core), :], dst_ref=near.at[slot],
            send_sem=s1_send, recv_sem=s1_recv.at[slot], device_id={"dp": partner}, device_id_type=MESH)

    def s2(j, k):
        return pltpu.make_async_remote_copy(
            src_ref=chip.at[j, k], dst_ref=far.at[j, k], send_sem=s2_send.at[j, k], recv_sem=s2_recv.at[j, k],
            device_id={"dp": across}, device_id_type=MESH)

    def places(layer, j):
        slot, index = 2 * layer + lax.rem(j, 2), layer * n + j
        return [
            (total.at[slot], g_hbm.at[index, :, half_of(core), :], slot, index),
            (total_d.at[slot], gd_hbm.at[index, :, half_of(core)], 4 + slot, 2 * n + index),
        ]

    def s3(layer, j):
        return [
            pltpu.make_async_remote_copy(
                src_ref=src, dst_ref=dst, send_sem=s3_send.at[slot], recv_sem=s3_recv.at[index], device_id={"dp": partner}, device_id_type=MESH)
            for src, dst, slot, index in places(layer, j)
        ]

    def put(layer, j):
        return [pltpu.make_async_copy(src, dst, put_sem.at[slot]) for src, dst, slot, _ in places(layer, j)]

    def drained(layer, j):
        for copy in s3(layer, j):
            copy.wait_send()
        for copy in put(layer, j):
            copy.wait()

    def leave(layer, j, k):
        if k > 0:
            s3(layer, j)[k - 1].start()
            put(layer, j)[k - 1].start()

    def free_total(layer, j):
        @pl.when(j >= 2)
        def _():
            drained(layer, j - 2)

    def deliver(layer, j, new, k):
        wide = new.astype(F32)
        if k == 2:
            total_d[2 * layer + lax.rem(j, 2)] = wide.T.astype(BF16)
        else:
            total[2 * layer + lax.rem(j, 2), k] = new
        ssv[...] += jnp.sum((wide * wide).reshape(half // 8, 8, J), 0)

    def keep(j):
        return pltpu.make_async_copy(grad, own_hbm.at[j], own_sem)

    most, left, right = pl.ds(0, tokens), pl.ds(0, d), pl.ds(d, d)
    hand = {
        "acc": [(md_hbm.at[1, most, :], acc)],
        "h": [(wd_hbm.at[1, most, :], h)],
        "a": [(wd_hbm.at[0, most, :], a)],
        "dh": [(wg_hbm.at[1, :, left], dh.at[left, :]), (wg_hbm.at[1, :, right], dh.at[right, :])],
        "at": [(wg_hbm.at[0, :, most], at)],
        "dht": [(wu_hbm.at[0, :, most], dht)],
    }
    hand = {name: [(*pair, k) for pair in pairs] for k, (name, pairs) in enumerate(hand.items())}
    hand["dh"][1] = (*hand["dh"][1][:2], len(hand))

    near_n = tokens // J
    hand["chip"] = [
        (wu_hbm.at[1, pl.ds(k * half, half), pl.ds(j * J, J)], chip.at[j, k], 7 + 2 * j + k) for j in range(near_n) for k in range(2)
    ]

    def handed(*names):
        return [pltpu.make_async_copy(src, dst, hand_sem.at[k]) for name in names for src, dst, k in hand[name]]

    def step(t, _):
        p, j = t // n, lax.rem(t, n)

        @pl.when(jnp.logical_and(p == 1, j == 0))
        def _():
            keep(n - 1).wait()
            lax.fori_loop(0, blocks, to_layer_0, 0)
            get = pltpu.make_async_copy(x_hbm, h, x_sem.at[0])
            get.start()
            get.wait()

        @pl.when(jnp.logical_and(p == 2, j == 0))
        def _():
            to_across(dy_hbm, far_dy, 0).wait()
            to_across(h_hbm, far_h, 1).wait()
            get = pltpu.make_async_copy(far_h, h, x_sem.at[0])
            get.start()
            get_too = pltpu.make_async_copy(far_dy, dh, x_sem.at[1])
            get_too.start()
            get.wait()
            get_too.wait()

        @pl.when(j == 0)
        def _():
            lax.fori_loop(0, blocks, begin, 0)

        @pl.when(jnp.logical_and(p == 2, j == 0))
        def _():
            for copy in handed("acc", "h"):
                copy.start()

        slot = next_weights(n + t)

        @pl.when(p == 2)
        def _():
            pltpu.make_async_copy(own_hbm.at[j], mine, own_sem).start()

        def block(r, _):
            here = rows(r)
            both = dot(a[here, :], wgu[slot])
            gate, up = both[:, :J], both[:, J:]
            by_act = dot_nt(dh[here, :], wd[slot]).astype(BF16).astype(F32)
            s = jax.nn.sigmoid(gate)
            silu = gate * s
            act[here, :] = (silu * up).astype(BF16)
            dgu[here, J:] = (by_act * silu).astype(BF16)
            dgu[here, :J] = (by_act * up * (s + silu * (1.0 - s))).astype(BF16)
            return 0

        lax.fori_loop(0, blocks, block, 0, unroll=True)

        @pl.when(t == 3 * n - 1)
        def _():
            for copy in handed("a", "dh"):
                copy.start()

        @pl.when(jnp.logical_and(p == 0, j > 0))
        def _():
            keep(j - 1).wait()

        def rest(i, _):
            here = half_of(lax.rem(1 - core + i, 2))
            both = dot(at[here, :], dgu[...]).astype(BF16)
            grad[0, here, :] = both[:, :J]
            grad[1, here, :] = both[:, J:]
            grad[2, here, :] = dot(dht[here, :], act[...]).astype(BF16)

            @pl.when(jnp.logical_and(i == 0, p == 2))
            def _():
                pltpu.make_async_copy(own_hbm.at[j], mine, own_sem).wait()
                for k in range(3):
                    grad[k, here, :] = (grad[k, here, :].astype(F32) + mine[k, here, :].astype(F32)).astype(BF16)

            @pl.when(jnp.logical_and(i == 0, p >= 1))
            def _():
                s1(t - n).start()

            return 0

        lax.fori_loop(0, 2, rest, 0)

        @pl.when(t == 3 * n - 1)
        def _():
            for copy in handed("at", "dht", "chip"):
                copy.start()

        @pl.when(p == 0)
        def _():
            keep(j).start()

            def back(r, _):
                acc[rows(r), :] += dot_nt(dgu[rows(r), :], wgu[slot])
                return 0

            lax.fori_loop(0, blocks, back, 0, unroll=True)

        @pl.when(p == 1)
        def _():
            s1(t - n).wait()
            for k in range(3):
                chip[j, k] = (grad[k, half_of(core), :].astype(F32) + near[lax.rem(t - n, 2), k].astype(F32)).astype(BF16)
                s2(j, k).start()

        @pl.when(p == 2)
        def _():
            free_total(1, j)
            s1(t - n).wait()
            for k in range(3):
                new = grad[k, half_of(core), :].astype(F32) + mine[k, half_of(core), :].astype(F32)
                deliver(1, j, (new + near[lax.rem(t - n, 2), k].astype(F32)).astype(BF16), k)
                leave(1, j, k)
            free_total(0, j)
            for k in range(3):
                s2(j, k).wait()
                deliver(0, j, (chip[j, k].astype(F32) + far[j, k].astype(F32)).astype(BF16), k)
                leave(0, j, k)

        return 0

    lax.fori_loop(0, 3 * n, step, 0)
    share = pltpu.make_async_remote_copy(
        src_ref=ssv, dst_ref=ssr, send_sem=ss_sem.at[0], recv_sem=ss_sem.at[1], device_id={"dp": partner}, device_id_type=MESH)
    share.start()
    for layer in range(2):
        for j in (n - 2, n - 1):
            drained(layer, j)

    def arrived(j, _):
        for copy in s3(0, j) + s3(1, j):
            copy.wait_recv()
        return 0

    lax.fori_loop(0, n, arrived, 0)
    share.wait()
    for copy in handed(*hand):
        copy.wait()
    ss_ref[...] = ssv[...] + ssr[...]


def call_gradients(x, dy, wg, wu, wd, md):
    tokens, d = x.shape
    n = wg.shape[2] // J
    half = d // 2
    hbm = pl.BlockSpec(memory_space=pltpu.HBM)
    vmem = pl.BlockSpec(memory_space=pltpu.VMEM)
    dma = pltpu.SemaphoreType.DMA
    part = (3, half, J)
    operands = [pltpu.with_memory_space_constraint(one, pltpu.HBM) for one in (x, dy, wg, wu, wd, md)]
    g, gd, ss, _, _, _, _, *kept = pl.pallas_call(
        gradients,
        name="gradients",
        out_shape=(
            pltpu.HBM((2 * n, 2, d, J), BF16), pltpu.HBM((2 * n, J, d), BF16), jax.ShapeDtypeStruct((8, J), F32),
            *[pltpu.HBM((tokens, d), BF16)] * 3, pltpu.HBM((n, 3, d, J), BF16),
            pltpu.VMEM((tokens, d), BF16), pltpu.VMEM((tokens, d), BF16), pltpu.VMEM((d, tokens), BF16),
            pltpu.VMEM((tokens, d), BF16), pltpu.VMEM((d, tokens), BF16), pltpu.VMEM((tokens, d), F32), pltpu.VMEM((n, *part), BF16),
        ),
        in_specs=[hbm] * 6,
        out_specs=(hbm, hbm, vmem, hbm, hbm, hbm, hbm, *[vmem] * 7),
        scratch_shapes=[
            pltpu.VMEM((tokens, J), BF16), pltpu.VMEM((tokens, 2 * J), BF16),
            pltpu.VMEM((2, d, 2 * J), BF16), pltpu.VMEM((2, J, d), BF16),
            pltpu.VMEM((3, d, J), BF16), pltpu.VMEM((3, d, J), BF16), pltpu.VMEM((2, *part), BF16), pltpu.VMEM((n, *part), BF16), pltpu.VMEM((4, 2, half, J), BF16), pltpu.VMEM((4, J, half), BF16),
            pltpu.VMEM((8, J), F32), pltpu.VMEM((8, J), F32),
            dma((3, 2)), dma((2,)), dma, dma((2,)), dma((2,)), dma, dma((2,)), dma((n, 3)), dma((n, 3)), dma((8,)), dma((4 * n,)), dma((8,)), dma((2,)), dma((7 + 2 * (tokens // J),)),
        ],
        compiler_params=pltpu.CompilerParams(collective_id=0, has_side_effects=True, vmem_limit_bytes=VMEM_LIMIT - HANDED),
    )(*operands)
    return (g, gd), ss, kept


def adamw(count, near, ss, h, a, at, dh, dht, acc, ups, g, gd, wg, wu, wd, mg, mu, md, vg, vu, vd, *outs):
    d = 2 * wg.shape[1]
    part = pl.program_id(2)
    row, row_d = pl.program_id(2) * wg.shape[1], pl.program_id(2) * wd.shape[1]
    layer, j = pl.program_id(0), pl.program_id(1)
    here = jnp.minimum(j, near - 1)
    chunk = pl.ds(pl.multiple_of(here * J, J), J)
    kept, first = j < near, layer == 0
    squares = jnp.sum(jnp.sum(ss[...], 0, keepdims=True), 1, keepdims=True)
    factor = jnp.minimum(1.0, 0.5 * lax.rsqrt(squares / count + 1e-30))

    def take(k, size, w, m, v):
        def some(i, _):
            piece = pl.ds(pl.multiple_of(i * size, size), size)
            mine = (gd[0, piece, :] if k == 2 else g[0, k, piece, :]).astype(F32) * factor
            new_m = 0.9 * m(piece) + 0.1 * mine
            new_v = 0.95 * v(piece) + 0.05 * mine * mine
            old = w(piece).astype(F32)
            outs[k][0, piece, :] = (old - 0.02 * (new_m * lax.rsqrt(new_v + 1e-8) + 0.1 * old)).astype(BF16)
            outs[3 + k][0, piece, :] = new_m
            outs[6 + k][0, piece, :] = new_v
            return 0

        lax.fori_loop(0, outs[k].shape[1] // size, some, 0, unroll=2)

    def rows_of(ref):
        return lambda piece: ref[0, piece, :]

    def rows(piece):
        return pl.ds(pl.multiple_of(row + piece.start, WIDE), WIDE)

    def of_chunk(ref):
        return lambda piece: ref[pl.ds(pl.multiple_of(here * J + row_d + piece.start, TALL), TALL), :]

    gate, up, down = (rows_of(mg), rows_of(vg)), (rows_of(mu), rows_of(vu)), (rows_of(md), rows_of(vd))

    @pl.when(jnp.logical_and(kept, first))
    def _():
        take(0, WIDE, lambda piece: at[rows(piece), chunk], *gate)
        take(1, WIDE, lambda piece: dht[rows(piece), chunk], *up)
        take(2, TALL, of_chunk(a), *down)

    @pl.when(jnp.logical_and(kept, layer == 1))
    def _():
        across = d // J
        cols = pl.ds(pl.multiple_of(here % across * J, J), J)
        take(0, WIDE, lambda piece: dh[pl.ds(pl.multiple_of(here // across * d + row + piece.start, WIDE), WIDE), cols], *gate)
        take(1, WIDE, lambda piece: ups[here, part, piece, :], *up)
        take(2, TALL, of_chunk(h), of_chunk(acc), down[1])

    @pl.when(j >= near)
    def _():
        take(0, WIDE, rows_of(wg), *gate)
        take(1, WIDE, rows_of(wu), *up)
        take(2, TALL, rows_of(wd), *down)


def call_adamw(ss, kept, g, weights, m, v):
    layers, d, ff = weights[0].shape
    n = ff // J
    near = kept[0].shape[0] // J
    vmem = pl.BlockSpec(memory_space=pltpu.VMEM)

    def there(l, j):
        return jnp.maximum(j, near)

    def there_1(l, j):
        return jnp.where(l == 1, jnp.maximum(j, near), j)

    def own(l, j):
        return j

    def wide(at, mode=None):
        return pl.BlockSpec((1, d // 2, J), lambda l, j, i: (l, jnp.where(at(l, j) == j, i, 0), at(l, j)), pipeline_mode=mode)

    def tall(at, mode=None):
        return pl.BlockSpec((1, J // 2, d), lambda l, j, i: (l, 2 * at(l, j) + jnp.where(at(l, j) == j, i, 0), 0), pipeline_mode=mode)

    count = float(3 * layers * d * ff)
    mode, mode_out = pl.Buffered(4), pl.Buffered(2)
    kept = [pltpu.with_memory_space_constraint(one, pltpu.VMEM) for one in kept]
    gs = [pl.BlockSpec((1, 2, d // 2, J), lambda l, j, i: (l * n + j, 0, i, 0), pipeline_mode=mode),
          pl.BlockSpec((1, J // 2, d), lambda l, j, i: (l * n + j, i, 0), pipeline_mode=mode)]
    hbm = pl.BlockSpec(memory_space=pltpu.HBM)

    def kernel(ss, h, a, at, dh, dht, acc, ups, *refs):
        pltpu.emit_pipeline(
            lambda *blocks: adamw(count, near, ss, h, a, at, dh, dht, acc, ups, *blocks),
            grid=(layers, n, 2),
            in_specs=[*gs, wide(there), wide(there), tall(there), wide(own, mode), wide(own, mode), tall(there_1, mode),
                      wide(own, mode), wide(own, mode), tall(own, mode)],
            out_specs=[wide(own, mode_out), wide(own, mode_out), tall(own, mode_out)] * 3,
        )(*refs)

    arrays = [pltpu.with_memory_space_constraint(one, pltpu.HBM) for one in (*g, *weights, *m, *v)]
    return pl.pallas_call(
        kernel,
        name="adamw",
        out_shape=[pltpu.HBM(w.shape, t) for t in (BF16, F32, F32) for w in weights],
        in_specs=[vmem] * 8 + [hbm] * len(arrays),
        out_specs=[hbm] * 9,
        compiler_params=pltpu.CompilerParams(vmem_limit_bytes=VMEM_LIMIT - HANDED),
    )(ss, *kept, *arrays)


def solution(mesh):
    def step(x, dy, *arrays):
        weights, m, v = (arrays[i : i + 3] for i in (0, 3, 6))
        g, ss, kept = call_gradients(x[0], dy[0], *weights, m[2])
        return tuple(call_adamw(ss, kept, g, weights, m, v))

    return jax.shard_map(
        step,
        mesh=mesh,
        in_specs=(P(("rep", "dp"), None, None),) * 2 + (P(None, None, None),) * 9,
        out_specs=(P("rep", None, None),) * 9,
        check_vma=False,
    )
```
